256 devices in a mesh: dp: 4 (over x), expert: 64 (over y, z, core).
Axes of the slice: x: 4, y: 4, z: 8, core: 2. Of those that a mesh axis runs over, the one named last changes fastest.
Arguments:
- tokens: bfloat16 [32768, 2048], P(('dp', 'expert')), may hold values from -6 to 6
- routes: int32 [32768, 8], P(('dp', 'expert')), may hold values from 0 to 127, all different within a row
- route_weight: float32 [32768, 8], P(('dp', 'expert')), may hold values from 0.05 to 0.5
- bias: float32 [128], replicated, may hold values from -3 to 3
- w_gate: bfloat16 [128, 768, 2048], P('expert', 'dp'), may hold values from -0.125 to 0.125
- w_up: bfloat16 [128, 768, 2048], P('expert', 'dp'), may hold values from -0.125 to 0.125
- w_down: bfloat16 [128, 768, 2048], P('expert', 'dp'), may hold values from -0.21875 to 0.21875
Outputs:
- mixed: bfloat16 [32768, 2048], P(('dp', 'expert'))
- new_bias: float32 [128], replicated
- counts: int32 [128], replicated
The draws below stay inside these ranges and needn't reach their ends.
Inputs may be any that keep to these rules, and one draw needn't show every extreme that they name: `routes`: each token names 8 different experts.
All inputs are finite; a program needn't handle non-finite values.
Results may differ from the reference program's by a relative error of at most 0.0057.
Values may be sent and summed in bfloat16 or wider, within the bound.
A program may use at most 128 MiB of HBM per device.

```python
import jax
import jax.numpy as jnp
from jax import lax

D = 2048
FF = 768
TOP = 8
TOK_DEV = 128
EXPERTS = 128
TOKENS = 32768
CAP = 10


def level_of(rng, extent, shards, smallest, top_value):
    loudness, own = 1.0, jax.random.fold_in(rng, 6)
    for position, shards_of in shards:
        heights = jnp.exp(jax.random.uniform(jax.random.fold_in(own, position), (shards_of,), jnp.float32, smallest / len(shards), top_value / len(shards)))
        loudness = loudness * jnp.repeat(heights, extent[position] // shards_of).reshape([-1 if axis == position else 1 for axis in range(len(extent))])
    return loudness


def different_ones(key, rows, amount, top, lift):
    order = jax.random.permutation(jax.random.fold_in(key, 1), amount)
    favour = order
    for power in range(3):
        favour = favour * favour // amount
    favour = favour * lift // amount
    lots = jax.random.randint(jax.random.fold_in(key, 2), (rows, amount), 0, 4096) + favour
    holders = jax.random.permutation(jax.random.fold_in(key, 3), rows)[jnp.arange(amount) % rows]
    lots = jnp.where(jnp.arange(rows)[:, None] == holders[None, :], 1 << 14, lots)
    merit = lots * amount + jnp.arange(amount)
    return lax.top_k(merit.astype(jnp.int32), top)[1].astype(jnp.int32)


def scatter_about(own_key, extent, width, reach, shards=(), held_as=jnp.bfloat16):
    drawn = jax.random.normal(own_key, extent, jnp.float32) * width
    if len(shards) > 0:
        drawn = level_of(own_key, extent, shards, -0.22, 0.18) * drawn
    return jnp.clip(drawn, min=-reach, max=reach).astype(held_as)


def setup_inputs(seed: int = 0) -> dict:
    key_of = jax.random.split(jax.random.key(seed), 8)
    tokens = scatter_about(key_of[0], (TOKENS, D), 1.0, 6.0, ((0, 256),))
    routes = different_ones(key_of[1], TOKENS, EXPERTS, TOP, 512)
    route_weight = jnp.clip(0.05 + 0.45 * jax.random.uniform(key_of[2], (TOKENS, TOP), jnp.float32) ** level_of(key_of[2], (TOKENS, TOP), ((0, 256),), -0.2, 0.2), 0.05, 0.5)
    bias = scatter_about(key_of[3], (EXPERTS,), 0.5, 3.0, (), jnp.float32)
    w_gate = scatter_about(key_of[4], (EXPERTS, FF, D), D ** -0.5, 0.125, ((0, 64), (1, 4)))
    w_up = scatter_about(key_of[5], (EXPERTS, FF, D), D ** -0.5, 0.125, ((0, 64), (1, 4)))
    w_down = scatter_about(key_of[6], (EXPERTS, FF, D), FF ** -0.5, 0.21875, ((0, 64), (1, 4)))
    return dict(tokens=tokens, routes=routes, route_weight=route_weight, bias=bias, w_gate=w_gate, w_up=w_up, w_down=w_down)


bias_rate = 0.05


def reference(tokens, routes, route_weight, bias, w_gate, w_up, w_down):
    sources = TOKENS // TOK_DEV
    entries = TOK_DEV * TOP
    block_routes = routes.reshape(sources, entries)
    labels = jnp.arange(EXPERTS, dtype=jnp.int32)

    def rank_block(block_row):
        picked = (block_row[:, None] == labels[None, :]).astype(jnp.int32)
        running = jnp.cumsum(picked, axis=0) - picked
        return jnp.sum(running * picked, axis=1).astype(jnp.int32), jnp.sum(picked, axis=0).astype(jnp.int32)

    slot_rank, block_counts = lax.map(rank_block, block_routes)
    counts = jnp.sum(block_counts, axis=0).astype(jnp.int32)
    kept_mask = slot_rank < CAP
    source_index = jnp.arange(sources, dtype=jnp.int32)[:, None]
    token_index = (source_index * TOK_DEV + jnp.arange(entries, dtype=jnp.int32)[None, :] // TOP).astype(jnp.int32)
    slot_total = EXPERTS * sources * CAP
    slot_index = jnp.where(kept_mask, block_routes * (sources * CAP) + source_index * CAP + slot_rank, slot_total).astype(jnp.int32)
    token_table = jnp.zeros((slot_total + 1,), jnp.int32).at[slot_index.reshape(-1)].set(token_index.reshape(-1))
    token_table = token_table[:slot_total].reshape(EXPERTS, sources * CAP)
    entry_weight = jnp.where(kept_mask, route_weight.reshape(sources, entries), jnp.float32(0.0)).astype(jnp.float32)
    weight_table = jnp.zeros((slot_total + 1,), jnp.float32).at[slot_index.reshape(-1)].set(entry_weight.reshape(-1))
    weight_table = weight_table[:slot_total].reshape(EXPERTS, sources * CAP)

    def one_expert(carry_sum, expert_items):
        slot_tokens, slot_weights, gate_w, up_w, down_w = expert_items
        picked_rows = tokens[slot_tokens]
        gate_act = lax.dot_general(picked_rows, gate_w, (((1,), (1,)), ((), ())), preferred_element_type=jnp.float32)
        up_act = lax.dot_general(picked_rows, up_w, (((1,), (1,)), ((), ())), preferred_element_type=jnp.float32)
        hidden = (jax.nn.silu(gate_act) * up_act).astype(jnp.bfloat16)
        expert_out = jnp.dot(hidden, down_w, preferred_element_type=jnp.float32).astype(jnp.bfloat16)
        return carry_sum.at[slot_tokens].add(expert_out.astype(jnp.float32) * slot_weights[:, None]), None

    summed, _ = lax.scan(one_expert, jnp.zeros((TOKENS, D), jnp.float32), (token_table, weight_table, w_gate, w_up, w_down))
    mixed = summed.astype(jnp.bfloat16)
    new_bias = bias + bias_rate * jnp.sign((TOKENS * TOP - EXPERTS * counts).astype(jnp.float32))
    return mixed, new_bias, counts
```

```python
import functools

import jax
import jax.numpy as jnp
from jax import lax
from jax.experimental import pallas as pl
from jax.experimental.pallas import tpu as pltpu
from jax.sharding import Mesh
from jax.sharding import PartitionSpec as P

EXPERT = ("expert_0", "expert_1", "expert_2")
DP_EXPERT = ("dp", "expert_0", "expert_1", "expert_2")
MESH = pl.DeviceIdType.MESH
BF16, F32 = jnp.bfloat16, jnp.float32

NX, NY, NZ, NCORE = 4, 4, 8, 2
PER = 2
CAP = 10
NS = NY * NCORE
SLOTS = CAP * NZ
NC = 8
bias_rate = 0.05

NT = (((1,), (1,)), ((), ()))


def wrap(v, n):
    return lax.rem(v + 2 * n, n)


def kernel(
    meta_ref, bias_ref, tok_ref, wg_ref, wu_ref, wd_ref,
    out_ref, cnt_ref, nb_ref,
    xb, pm, wh, wl, sb, rb, cb, wgu, wdn, hid, rl1, rl2, rsb, meta, keys, wks, csend, crecv,
    loc_s, tok_s, wdl_s, meta_ss, meta_rs, c_ss, c_rs,
    z_ss, z_rs, y1_ss, y1_rs, l1_rs, f1_ss, y2_ss, y2_rs, l2_rs, f2_ss, r_ss, r_rs,
    g_ss, g_rs, d_ss, d_rs,
):
    x, y = lax.axis_index("dp"), lax.axis_index("expert_0")
    z, c = lax.axis_index("expert_1"), lax.axis_index("expert_2")
    feat = tok_ref.shape[1]
    width = feat // NC
    tok = tok_ref.shape[0]
    ff = wg_ref.shape[1]
    xp, xm = wrap(x + 1, NX), wrap(x - 1, NX)
    yp, ym = wrap(y + 1, NY), wrap(y - 1, NY)
    other = 1 - c
    mine = y * NCORE + c
    home = (x, y, z, c)

    def rcopy(src, dst, ss, rs, to):
        return pltpu.make_async_remote_copy(
            src_ref=src, dst_ref=dst, send_sem=ss, recv_sem=rs, device_id=to, device_id_type=MESH
        )

    def got(ref, sem):
        rcopy(ref, ref, sem, sem, (xp, y, z, c)).wait_recv()

    def sent(ref, sem):
        rcopy(ref, ref, sem, sem, (xp, y, z, c)).wait_send()

    own_g = [
        pltpu.make_async_copy(wg_ref, wgu.at[0, :, x], loc_s.at[0]),
        pltpu.make_async_copy(wu_ref, wgu.at[1, :, x], loc_s.at[1]),
    ]
    own_g[0].start()
    own_g[1].start()

    def columns(k):
        return pl.ds(pl.multiple_of(k * width, width), width)

    def tok_copy(k):
        return pltpu.make_async_copy(tok_ref.at[:, columns(k)], xb.at[k, z], tok_s.at[k])

    def wd_copy(k):
        return pltpu.make_async_copy(wd_ref.at[:, :, columns(k)], wdn.at[k, :, x], wdl_s.at[k])

    @pl.loop(0, NC)
    def _(k):
        tok_copy(k).start()

    @pl.loop(0, NC)
    def _(k):
        wd_copy(k).start()

    barrier = pltpu.get_barrier_semaphore()
    peers = [(xp, y, z, c), (xm, y, z, c), (x, y, z, other)]
    peers += [(x, yy, z, cc) for yy in (yp, ym) for cc in range(NCORE)]
    peers += [(x, y, wrap(z + o, NZ), c) for o in range(1, NZ)]
    for p in peers:
        pl.semaphore_signal(barrier, inc=1, device_id=p, device_id_type=MESH)
    pl.semaphore_wait(barrier, len(peers))

    for o in range(1, NZ):
        rcopy(meta_ref, meta.at[z], meta_ss, meta_rs, (x, y, wrap(z + o, NZ), c)).start()
    meta[z] = meta_ref[...]

    def z_hop(k, h):
        s = 1 - 2 * lax.rem(k, 2)
        far = wrap(z - s * (h - 1), NZ)
        near = wrap(z + s * (h - 1), NZ)
        if h >= 2:
            got(xb.at[k, far], z_rs.at[k, 0, h - 2])
        rcopy(
            xb.at[k, far], xb.at[k, far], z_ss.at[k], z_rs.at[k, 0, h - 1],
            (x, y, wrap(z + s, NZ), c),
        ).start()
        if h >= 4:
            return
        if h >= 2:
            got(xb.at[k, near], z_rs.at[k, 1, h - 2])
        rcopy(
            xb.at[k, near], xb.at[k, near], z_ss.at[k], z_rs.at[k, 1, h - 1],
            (x, y, wrap(z - s, NZ), c),
        ).start()

    def z_own(k):
        tok_copy(k).wait()
        z_hop(k, 1)

    z_own(0)
    z_own(1)

    own_g[0].wait()
    own_g[1].wait()

    def g_piece(w, j, xs):
        return wgu.at[w, j, xs]

    for j in range(PER):
        for w in range(2):
            a, b = g_piece(w, j, x), g_piece(w, 1 - j, x)
            rcopy(a, a, g_ss.at[0, w * PER + j], g_rs.at[0, w * PER + j], (xp, y, z, c)).start()
            i = w * PER + 1 - j
            rcopy(b, b, g_ss.at[1, i], g_rs.at[1, i], (xm, y, z, c)).start()

    def g_relay(w):
        got(g_piece(w, 0, xm), g_rs.at[0, w * PER])
        a = g_piece(w, 0, xm)
        rcopy(a, a, g_ss.at[2, w], g_rs.at[2, w], (xp, y, z, c)).start()
        got(g_piece(w, 1, xp), g_rs.at[1, w * PER + 1])
        b = g_piece(w, 1, xp)
        rcopy(b, b, g_ss.at[3, w], g_rs.at[3, w], (xm, y, z, c)).start()

    got(meta.at[pl.ds(0, NZ - 1)], meta_rs)
    row = lax.broadcasted_iota(jnp.int32, (NS * PER, tok), 0)
    expert = ((row // 4) * (NZ * 4) + z * 4 + row % 4).astype(F32)
    before = (
        lax.broadcasted_iota(jnp.int32, (tok, tok), 0)
        < lax.broadcasted_iota(jnp.int32, (tok, tok), 1)
    ).astype(F32).astype(BF16)
    slot_row = lax.broadcasted_iota(jnp.int32, (NS * PER, SLOTS, tok), 1).astype(F32)

    @pl.loop(0, NZ)
    def _(b):
        hit = jnp.zeros((NS * PER, tok), F32)
        weight = jnp.zeros((NS * PER, tok), F32)
        for k in range(8):
            same = meta[b, k : k + 1, :] == expert
            hit = jnp.where(same, 1.0, hit)
            weight = jnp.where(same, meta[b, 8 + k : 9 + k, :], weight)
        rank = jnp.dot(hit.astype(BF16), before, preferred_element_type=F32)
        key = jnp.where(hit > 0.0, rank * NZ + b.astype(F32), -1.0)
        keys[b] = key
        wks[b] = weight
        pick = jnp.where(key[:, None, :] == slot_row, 1.0, 0.0)
        at = pl.ds(pl.multiple_of(b * tok, tok), tok)
        pm[:, at] = pick.reshape(NS * PER * SLOTS, tok).astype(BF16)

    def y_send(k, src, dst, rl, ss, rs, ls):
        rcopy(src.at[k, y * NCORE + other], dst.at[k, mine], ss.at[k], rs.at[k], (x, y, z, other)).start()
        for cc, yf, to in ((0, yp, 0), (1, ym, 1)):
            opp = wrap(y + 2, NY)
            rcopy(src.at[k, opp * NCORE + cc], rl.at[k, to], ss.at[k], ls.at[k, to], (x, yf, z, c)).start()
        for yy in (yp, ym):
            for cc in range(NCORE):
                rcopy(src.at[k, yy * NCORE + cc], dst.at[k, mine], ss.at[k], rs.at[k], (x, yy, z, cc)).start()

    def y_forward(k, dst, rl, fs, rs, ls):
        got(rl.at[k, 0], ls.at[k, 0])
        rcopy(rl.at[k, 0], dst.at[k, ym * NCORE + c], fs.at[k], rs.at[k], (x, yp, z, 0)).start()
        got(rl.at[k, 1], ls.at[k, 1])
        rcopy(rl.at[k, 1], dst.at[k, yp * NCORE + c], fs.at[k], rs.at[k], (x, ym, z, 1)).start()

    def pick_rows(k):
        s = 1 - 2 * lax.rem(k, 2)
        got(xb.at[k, wrap(z + 4, NZ)], z_rs.at[k, 0, 3])
        got(xb.at[k, wrap(z + 3 * s, NZ)], z_rs.at[k, 1, 2])
        half = NS * PER * SLOTS // 2

        @pl.loop(0, 2)
        def _(p):
            rows = pm[pl.ds(pl.multiple_of(p * half, half), half), :]
            picked = jnp.dot(rows, xb[k].reshape(NZ * tok, width), preferred_element_type=F32)
            picked = picked.astype(BF16).reshape(NS // 2, PER, SLOTS, width)
            sb[k, pl.ds(p * (NS // 2), NS // 2)] = picked

        rb[k, mine] = sb[k, mine]
        y_send(k, sb, rb, rl1, y1_ss, y1_rs, l1_rs)

    def guarded(k, fn):
        @pl.when(jnp.logical_and(k >= 0, k < NC))
        def _():
            fn(k)

    @pl.loop(0, NC + 4)
    def _(i):
        guarded(i - 2, lambda k: z_hop(k, 4))
        guarded(i - 1, lambda k: z_hop(k, 3))
        guarded(i, lambda k: z_hop(k, 2))
        guarded(i + 2, z_own)
        guarded(i - 3, pick_rows)
        guarded(i - 4, lambda k: y_forward(k, rb, rl1, f1_ss, y1_rs, l1_rs))

        @pl.when(i == 5)
        def _():
            g_relay(0)

        @pl.when(i == 8)
        def _():
            g_relay(1)

    def d_own(k):
        wd_copy(k).wait()
        a = wdn.at[k, :, x]
        rcopy(a, a, d_ss.at[k, 0], d_rs.at[k, 0], (xp, y, z, c)).start()
        rcopy(a, a, d_ss.at[k, 1], d_rs.at[k, 1], (xm, y, z, c)).start()

    def d_relay(k):
        got(wdn.at[k, :, xm], d_rs.at[k, 0])
        a = wdn.at[k, 0, xm]
        rcopy(a, a, d_ss.at[k, 2], d_rs.at[k, 2], (xp, y, z, c)).start()
        got(wdn.at[k, :, xp], d_rs.at[k, 1])
        b = wdn.at[k, 1, xp]
        rcopy(b, b, d_ss.at[k, 3], d_rs.at[k, 3], (xm, y, z, c)).start()

    d_own(0)
    d_own(1)

    expert_row = lax.broadcasted_iota(jnp.int32, (tok, tok), 0).astype(F32)

    def count(b, total):
        hit = jnp.zeros((tok, tok), F32)
        for k in range(8):
            hit = jnp.where(meta[b, k : k + 1, :] == expert_row, 1.0, hit)
        ones = jnp.ones((8, tok), BF16)
        return total + lax.dot_general(ones, hit.astype(BF16), NT, preferred_element_type=F32)

    total = lax.fori_loop(0, NZ, count, jnp.zeros((8, tok), F32))
    y1 = y + 1 - 2 * lax.rem(y, 2)
    x1 = x + 1 - 2 * lax.rem(x, 2)
    partners = [(x, y, z, other), (x, y1, z, c), (x, NY - 1 - y, z, c), (x1, y, z, c), (NX - 1 - x, y, z, c)]
    csend[0] = total

    @pl.loop(0, NZ)
    def _(b):
        same = keys[b][:, None, :] == slot_row
        placed = jnp.where(same, wks[b][:, None, :], 0.0).reshape(NS * PER * SLOTS, tok).T
        high = placed.astype(BF16)
        wh[b] = high
        wl[b] = (placed - high.astype(F32)).astype(BF16)

    for s, to in enumerate(partners):
        move = rcopy(csend.at[s], crecv.at[s], c_ss.at[s], c_rs.at[s], to)
        move.start()
        move.wait()
        total = csend[s] + crecv[s]
        if s + 1 < len(partners):
            csend[s + 1] = total
    totals = total[0:1]
    cnt_ref[...] = totals.astype(jnp.int32)
    over = float(tok * 8 * NX * NY * NZ * NCORE) - float(tok) * totals
    sign = jnp.where(over > 0.0, 1.0, jnp.where(over < 0.0, -1.0, 0.0))
    nb_ref[...] = bias_ref[...] + bias_rate * sign

    @pl.loop(0, NC)
    def _(k):
        got(rb.at[k, pl.ds(0, NS - 1)], y1_rs.at[k])
        sent(xb.at[k, pl.ds(0, NZ - 1)], z_ss.at[k])
        sent(sb.at[k, pl.ds(0, NS - 1)], y1_ss.at[k])
        sent(rl1.at[k], f1_ss.at[k])

    sent(meta.at[pl.ds(0, NZ - 1)], meta_ss)

    def hidden_of(xs):
        @pl.loop(0, 2 * PER)
        def _(t):
            j = t // 2
            part = pl.ds((t % 2) * (NS // 2), NS // 2)
            gate = up = None
            for k in range(NC):
                rows = rb[k, part, j].reshape(NS // 2 * SLOTS, width)
                cols = slice(k * width, (k + 1) * width)
                g = lax.dot_general(rows, wgu[0, j, xs, :, cols], NT, preferred_element_type=F32)
                u = lax.dot_general(rows, wgu[1, j, xs, :, cols], NT, preferred_element_type=F32)
                gate = g if gate is None else gate + g
                up = u if up is None else up + u
            act = (gate / (1.0 + jnp.exp(-gate)) * up).astype(BF16)
            half = NS // 2 * SLOTS
            hid[j, xs, pl.ds(pl.multiple_of((t % 2) * half, half), half), :] = act

    @pl.loop(0, NX)
    def _(step):
        off = step + (step // 2) * (1 - 2 * (step % 2))
        xs = wrap(x + off, NX)

        @pl.when(step == 1)
        def _():
            for i in (0, 2):
                got(g_piece(i // PER, i % PER, xp), g_rs.at[1, i])

        @pl.when(step == 2)
        def _():
            for i in (1, 3):
                got(g_piece(i // PER, i % PER, xm), g_rs.at[0, i])

        @pl.when(step == 3)
        def _():
            opp = wrap(x + 2, NX)
            for w in range(2):
                got(g_piece(w, 0, opp), g_rs.at[2, w])
                got(g_piece(w, 1, opp), g_rs.at[3, w])

        hidden_of(xs)

    def down(k):
        opp = wrap(x + 2, NX)
        got(wdn.at[k, 0, opp], d_rs.at[k, 2])
        got(wdn.at[k, 1, opp], d_rs.at[k, 3])

        @pl.loop(0, PER)
        def _(j):
            total = None
            for xs in range(NX):
                t = jnp.dot(hid[j, xs], wdn[k, j, xs], preferred_element_type=F32)
                total = t if total is None else total + t
            sb[k, :, j] = total.astype(BF16).reshape(NS, SLOTS, width)

        cb[k, mine] = sb[k, mine]
        y_send(k, sb, cb, rl2, y2_ss, y2_rs, l2_rs)

    def far_send(k, h):
        s = 1 - 2 * lax.rem(k, 2)
        t = wrap(z + (5 - h) * s, NZ)
        if h >= 2:
            got(rsb.at[k, 0, h - 2], r_rs.at[k, 0, h - 2])
            xb[k, t] = (xb[k, t].astype(F32) + rsb[k, 0, h - 2].astype(F32)).astype(BF16)
        rcopy(xb.at[k, t], rsb.at[k, 0, h - 1], r_ss.at[k], r_rs.at[k, 0, h - 1], (x, y, wrap(z + s, NZ), c)).start()

    def near_send(k, h):
        s = 1 - 2 * lax.rem(k, 2)
        t = wrap(z - (4 - h) * s, NZ)
        if h >= 2:
            got(rsb.at[k, 1, h - 2], r_rs.at[k, 1, h - 2])
            xb[k, t] = (xb[k, t].astype(F32) + rsb[k, 1, h - 2].astype(F32)).astype(BF16)
        rcopy(xb.at[k, t], rsb.at[k, 1, h - 1], r_ss.at[k], r_rs.at[k, 1, h - 1], (x, y, wrap(z - s, NZ), c)).start()

    def combine(k):
        got(cb.at[k, pl.ds(0, NS - 1)], y2_rs.at[k])

        @pl.loop(0, 2)
        def _(p):
            part = pl.ds(p * (NZ // 2), NZ // 2)
            served = cb[k].reshape(NS * PER * SLOTS, width)
            hi = wh[part].reshape(NZ // 2 * tok, NS * PER * SLOTS)
            lo = wl[part].reshape(NZ // 2 * tok, NS * PER * SLOTS)
            summed = jnp.dot(hi, served, preferred_element_type=F32)
            summed += jnp.dot(lo, served, preferred_element_type=F32)
            xb[k, part] = summed.astype(BF16).reshape(NZ // 2, tok, width)

        far_send(k, 1)
        near_send(k, 1)

    def both(k, h):
        far_send(k, h)
        near_send(k, h)

    def finish(k):
        got(rsb.at[k, 0, 3], r_rs.at[k, 0, 3])
        got(rsb.at[k, 1, 2], r_rs.at[k, 1, 2])
        value = xb[k, z].astype(F32) + rsb[k, 0, 3].astype(F32) + rsb[k, 1, 2].astype(F32)
        out_ref[:, columns(k)] = value.astype(BF16)

    def feed(k):
        d_relay(k)
        guarded(k + 2, d_own)

    @pl.loop(0, NC + 7)
    def _(i):
        guarded(i - 7, finish)
        guarded(i - 6, lambda k: far_send(k, 4))
        guarded(i - 5, lambda k: both(k, 3))
        guarded(i - 4, lambda k: both(k, 2))
        guarded(i - 3, combine)
        guarded(i - 2, lambda k: y_forward(k, cb, rl2, f2_ss, y2_rs, l2_rs))
        guarded(i, feed)
        guarded(i - 1, down)

    for i in range(2 * PER):
        w, j = i // PER, i % PER
        sent(g_piece(w, j, x), g_ss.at[0, i])
        sent(g_piece(w, j, x), g_ss.at[1, i])
    for w in range(2):
        sent(g_piece(w, 0, xm), g_ss.at[2, w])
        sent(g_piece(w, 1, xp), g_ss.at[3, w])

    @pl.loop(0, NC)
    def _(k):
        sent(wdn.at[k, :, x], d_ss.at[k, 0])
        sent(wdn.at[k, :, x], d_ss.at[k, 1])
        sent(wdn.at[k, 0, xm], d_ss.at[k, 2])
        sent(wdn.at[k, 1, xp], d_ss.at[k, 3])
        sent(sb.at[k, pl.ds(0, NS - 1)], y2_ss.at[k])
        sent(rl2.at[k], f2_ss.at[k])
        sent(xb.at[k, pl.ds(0, NZ - 1)], r_ss.at[k])


def body(tokens, routes, route_weight, bias, w_gate, w_up, w_down):
    tok, feat = tokens.shape
    per, ff, _ = w_gate.shape
    experts = bias.shape[0]
    width = feat // NC
    rows = NS * PER * SLOTS
    meta = jnp.concatenate([routes.T.astype(F32), route_weight.T], axis=0)
    vmem, anywhere = pl.BlockSpec(memory_space=pltpu.VMEM), pl.BlockSpec(memory_space=pl.ANY)
    dma = pltpu.SemaphoreType.DMA
    mixed, counts, new_bias = pl.pallas_call(
        kernel,
        out_shape=(
            jax.ShapeDtypeStruct((tok, feat), BF16),
            jax.ShapeDtypeStruct((1, experts), jnp.int32),
            jax.ShapeDtypeStruct((1, experts), F32),
        ),
        in_specs=[vmem, vmem, anywhere, anywhere, anywhere, anywhere],
        out_specs=(vmem, vmem, vmem),
        scratch_shapes=[
            pltpu.VMEM((NC, NZ, tok, width), BF16),
            pltpu.VMEM((rows, NZ * tok), BF16),
            pltpu.VMEM((NZ, tok, rows), BF16),
            pltpu.VMEM((NZ, tok, rows), BF16),
            pltpu.VMEM((NC, NS, PER, SLOTS, width), BF16),
            pltpu.VMEM((NC, NS, PER, SLOTS, width), BF16),
            pltpu.VMEM((NC, NS, PER, SLOTS, width), BF16),
            pltpu.VMEM((2, per, NX, ff, feat), BF16),
            pltpu.VMEM((NC, per, NX, ff, width), BF16),
            pltpu.VMEM((per, NX, NS * SLOTS, ff), BF16),
            pltpu.VMEM((NC, 2, PER, SLOTS, width), BF16),
            pltpu.VMEM((NC, 2, PER, SLOTS, width), BF16),
            pltpu.VMEM((NC, 2, 4, tok, width), BF16),
            pltpu.VMEM((NZ, 16, tok), F32),
            pltpu.VMEM((NZ, NS * PER, tok), F32),
            pltpu.VMEM((NZ, NS * PER, tok), F32),
            pltpu.VMEM((5, 8, tok), F32),
            pltpu.VMEM((5, 8, tok), F32),
            dma((2,)),
            dma((NC,)),
            dma((NC,)),
            dma,
            dma,
            dma((5,)),
            dma((5,)),
            dma((NC,)),
            dma((NC, 2, 4)),
            dma((NC,)),
            dma((NC,)),
            dma((NC, 2)),
            dma((NC,)),
            dma((NC,)),
            dma((NC,)),
            dma((NC, 2)),
            dma((NC,)),
            dma((NC,)),
            dma((NC, 2, 4)),
            dma((4, 4)),
            dma((4, 4)),
            dma((NC, 4)),
            dma((NC, 4)),
        ],
        compiler_params=pltpu.CompilerParams(
            collective_id=0, has_side_effects=True, vmem_limit_bytes=67_043_328
        ),
        name="moe_layer",
    )(meta, bias.reshape(1, experts), tokens, w_gate, w_up, w_down)
    return mixed, new_bias.reshape(experts), counts.reshape(experts)


def solution(mesh):
    torus = Mesh(mesh.devices.reshape(NX, NY, NZ, NCORE), DP_EXPERT)
    placed = (
        P(DP_EXPERT, None),
        P(DP_EXPERT, None),
        P(DP_EXPERT, None),
        P(),
        P(EXPERT, "dp", None),
        P(EXPERT, "dp", None),
        P(EXPERT, "dp", None),
    )
    return jax.shard_map(
        body, mesh=torus, in_specs=placed, out_specs=(P(DP_EXPERT, None), P(), P()), check_vma=False
    )
```

```python
import functools

import jax
import jax.numpy as jnp
from jax import lax
from jax.experimental import pallas as pl
from jax.experimental.pallas import tpu as pltpu
from jax.sharding import Mesh
from jax.sharding import PartitionSpec as P

EXPERT = ("expert_0", "expert_1", "expert_2")
DP_EXPERT = ("dp", "expert_0", "expert_1", "expert_2")
MESH = pl.DeviceIdType.MESH
BF16, F32 = jnp.bfloat16, jnp.float32

NX, NY, NZ, NCORE = 4, 4, 8, 2
PER = 2
CAP = 10
NS = NY * NCORE
SLOTS = CAP * NZ
NC = 8
bias_rate = 0.05

NT = (((1,), (1,)), ((), ()))


def wrap(v, n):
    return lax.rem(v + 2 * n, n)


def kernel(
    route_ref, weight_ref, tok_ref, wg_ref, wu_ref, wd_ref,
    out_ref, cnt_ref,
    xb, pm, wh, wl, sb, rb, cb, wgu, wdn, hid, rl1, rl2, rsb, mroute, mweight, keys, wks, csend, crecv, outb,
    loc_s, tok_s, wdl_s, out_s, meta_ss, meta_rs, c_ss, c_rs,
    z_ss, z_rs, y1_ss, y1_rs, l1_rs, f1_ss, y2_ss, y2_rs, l2_rs, f2_ss, r_ss, r_rs,
    g_ss, g_rs, d_ss, d_rs,
):
    x, y = lax.axis_index("dp"), lax.axis_index("expert_0")
    z, c = lax.axis_index("expert_1"), lax.axis_index("expert_2")
    feat = tok_ref.shape[1]
    width = feat // NC
    tok = tok_ref.shape[0]
    ff = wg_ref.shape[1]
    xp, xm = wrap(x + 1, NX), wrap(x - 1, NX)
    yp, ym = wrap(y + 1, NY), wrap(y - 1, NY)
    other = 1 - c
    mine = y * NCORE + c
    home = (x, y, z, c)

    def rcopy(src, dst, ss, rs, to):
        return pltpu.make_async_remote_copy(
            src_ref=src, dst_ref=dst, send_sem=ss, recv_sem=rs, device_id=to, device_id_type=MESH
        )

    def got(ref, sem):
        rcopy(ref, ref, sem, sem, (xp, y, z, c)).wait_recv()

    def sent(ref, sem):
        rcopy(ref, ref, sem, sem, (xp, y, z, c)).wait_send()

    own_g = [
        pltpu.make_async_copy(wg_ref, wgu.at[0, :, x], loc_s.at[0]),
        pltpu.make_async_copy(wu_ref, wgu.at[1, :, x], loc_s.at[1]),
    ]
    own_g[0].start()
    own_g[1].start()

    def columns(k):
        return pl.ds(pl.multiple_of(k * width, width), width)

    def tok_copy(k):
        return pltpu.make_async_copy(tok_ref.at[:, columns(k)], xb.at[k, z], tok_s.at[(k + NC - 1) // NC])

    def wd_copy(k):
        return pltpu.make_async_copy(wd_ref.at[:, :, columns(k)], wdn.at[k, :, x], wdl_s)

    @pl.loop(0, NC)
    def _(k):
        tok_copy(k).start()

    @pl.loop(0, NC)
    def _(k):
        wd_copy(k).start()

    barrier = pltpu.get_barrier_semaphore()
    peers = [(xp, y, z, c), (xm, y, z, c), (x, y, z, other)]
    peers += [(x, yy, z, cc) for yy in (yp, ym) for cc in range(NCORE)]
    peers += [(x, y, wrap(z + 1, NZ), c), (x, y, wrap(z - 1, NZ), c)]
    for p in peers:
        pl.semaphore_signal(barrier, inc=1, device_id=p, device_id_type=MESH)
    pl.semaphore_wait(barrier, len(peers))

    def g_piece(w, j, xs):
        return wgu.at[w, j, xs]

    def g_own(w, j):
        a = g_piece(w, j, x)
        rcopy(a, a, g_ss, g_rs.at[w, j, 0], (xp, y, z, c)).start()
        rcopy(a, a, g_ss, g_rs.at[w, j, 0], (xm, y, z, c)).start()

    def g_arrived(w, j):
        got(wgu.at[w, :, x], g_rs.at[w, j, 0])

    def halves(ref):
        rows = ref.shape[0] // 2
        return ref.at[pl.ds(0, rows)], ref.at[pl.ds(rows, rows)]

    def g_relay(w, j):
        g_arrived(w, j)
        a = halves(g_piece(w, j, xm))[0]
        rcopy(a, a, g_ss, g_rs.at[w, j, 1], (xp, y, z, c)).start()
        b = halves(g_piece(w, j, xp))[1]
        rcopy(b, b, g_ss, g_rs.at[w, j, 1], (xm, y, z, c)).start()

    own_g[0].wait()
    g_own(0, 0)
    own_g[1].wait()
    g_own(1, 0)

    def z_hop(k, h):
        s = 1 - 2 * lax.rem(k, 2)
        far = xb.at[k, wrap(z - s * (h - 1), NZ)]
        near = xb.at[k, wrap(z + s * (h - 1), NZ)]
        if h >= 2:
            got(xb.at[k, pl.ds(0, 2)], z_rs.at[k, h - 2])
        rcopy(far, far, z_ss, z_rs.at[k, h - 1], (x, y, wrap(z + s, NZ), c)).start()
        if h < 4:
            rcopy(near, near, z_ss, z_rs.at[k, h - 1], (x, y, wrap(z - s, NZ), c)).start()

    def m_hop(h):
        for a, (own, held) in enumerate(((route_ref, mroute), (weight_ref, mweight))):
            if h >= 2:
                got(held.at[pl.ds(0, 2)], meta_rs.at[a, h - 2])
            p, q = wrap(z - (h - 1), NZ), wrap(z + (h - 1), NZ)
            rcopy(
                own if h == 1 else held.at[p], held.at[p], meta_ss.at[a], meta_rs.at[a, h - 1],
                (x, y, wrap(z + 1, NZ), c),
            ).start()
            if h < 4:
                rcopy(
                    own if h == 1 else held.at[q], held.at[q], meta_ss.at[a], meta_rs.at[a, h - 1],
                    (x, y, wrap(z - 1, NZ), c),
                ).start()

    m_hop(1)
    mroute[z] = route_ref[...]
    mweight[z] = weight_ref[...]
    tok_copy(0).wait()
    z_hop(0, 1)
    m_hop(2)
    m_hop(3)
    got(xb.at[pl.ds(0, NC - 1), z], tok_s.at[1])
    z_hop(1, 1)
    m_hop(4)

    got(mroute.at[0], meta_rs.at[0, 3])
    got(mweight.at[0], meta_rs.at[1, 3])
    row = lax.broadcasted_iota(jnp.int32, (NS * PER, tok), 0)
    expert = (row // 4) * (NZ * 4) + z * 4 + row % 4
    before = (
        lax.broadcasted_iota(jnp.int32, (tok, tok), 0)
        < lax.broadcasted_iota(jnp.int32, (tok, tok), 1)
    ).astype(F32).astype(BF16)
    slot_row = lax.broadcasted_iota(jnp.int32, (NS * PER, SLOTS, tok), 1).astype(F32)

    @pl.loop(0, NZ)
    def _(b):
        hit = jnp.zeros((NS * PER, tok), F32)
        weight = jnp.zeros((NS * PER, tok), F32)
        for k in range(8):
            same = mroute[b, k : k + 1, :] == expert
            hit = jnp.where(same, 1.0, hit)
            weight = jnp.where(same, mweight[b, k : k + 1, :], weight)
        rank = jnp.dot(hit.astype(BF16), before, preferred_element_type=F32)
        key = jnp.where(hit > 0.0, rank * NZ + b.astype(F32), -1.0)
        keys[b] = key
        wks[b] = weight
        pick = jnp.where(key[:, None, :] == slot_row, 1.0, 0.0)
        at = pl.ds(pl.multiple_of(b * tok, tok), tok)
        pm[:, at] = pick.reshape(NS * PER * SLOTS, tok).astype(BF16)

    def y_send(src, dst, rl, ss, rs, ls):
        rcopy(src(y * NCORE + other), dst(mine), ss, rs, (x, y, z, other)).start()
        for cc, yf in ((0, yp), (1, ym)):
            opp = wrap(y + 2, NY)
            rcopy(src(opp * NCORE + cc), rl(cc), ss, ls, (x, yf, z, c)).start()
        for yy in (yp, ym):
            for cc in range(NCORE):
                rcopy(src(yy * NCORE + cc), dst(mine), ss, rs, (x, yy, z, cc)).start()

    def y_forward(dst, rl, landed, fs, rs, ls):
        got(landed, ls)
        rcopy(rl(0), dst(ym * NCORE + c), fs, rs, (x, yp, z, 0)).start()
        rcopy(rl(1), dst(yp * NCORE + c), fs, rs, (x, ym, z, 1)).start()

    def pick_rows(k):
        got(xb.at[k, 0], z_rs.at[k, 3])
        half = NS * PER * SLOTS // 2

        @pl.loop(0, 2)
        def _(p):
            rows = pm[pl.ds(pl.multiple_of(p * half, half), half), :]
            picked = jnp.dot(rows, xb[k].reshape(NZ * tok, width), preferred_element_type=F32)
            picked = picked.astype(BF16).reshape(NS // 2, PER, SLOTS, width)
            sb[k, pl.ds(p * (NS // 2), NS // 2)] = picked

        rb[k, mine] = sb[k, mine]
        y_send(
            lambda d: sb.at[k, d], lambda d: rb.at[k, d], lambda d: rl1.at[k, d],
            y1_ss, y1_rs.at[k], l1_rs.at[k],
        )

    def pass_rows(k):
        y_forward(
            lambda d: rb.at[k, d], lambda d: rl1.at[k, d], rl1.at[k], f1_ss, y1_rs.at[k], l1_rs.at[k]
        )

    def guarded(k, fn, first=0, last=NC):
        @pl.when(jnp.logical_and(k >= first, k < last))
        def _():
            fn(k)

    units, early = 2 * NC, NC // 2

    def unit(u):
        late = u // NC
        k = (1 - late) * (u % early) + late * (early + (u - NC + units) % NC // 2)
        j = (1 - late) * (u // early) + late * (u % 2)
        return k, j

    def d_own(u):
        k, j = unit(u)
        a = wdn.at[k, j, x]
        rcopy(a, a, d_ss, d_rs.at[u, 0], (xp, y, z, c)).start()
        rcopy(a, a, d_ss, d_rs.at[u, 0], (xm, y, z, c)).start()

    def d_relay(u):
        k, j = unit(u)
        got(wdn.at[k, :, x], d_rs.at[u, 0])
        a = halves(wdn.at[k, j, xm])[0]
        rcopy(a, a, d_ss, d_rs.at[u, 1], (xp, y, z, c)).start()
        b = halves(wdn.at[k, j, xp])[1]
        rcopy(b, b, d_ss, d_rs.at[u, 1], (xm, y, z, c)).start()

    expert_row = lax.broadcasted_iota(jnp.int32, (tok, tok), 0)

    def count(b, total):
        hit = jnp.zeros((tok, tok), F32)
        for k in range(8):
            hit = jnp.where(mroute[b, k : k + 1, :] == expert_row, 1.0, hit)
        ones = jnp.ones((8, tok), BF16)
        return total + lax.dot_general(ones, hit.astype(BF16), NT, preferred_element_type=F32)

    y1 = y + 1 - 2 * lax.rem(y, 2)
    x1 = x + 1 - 2 * lax.rem(x, 2)
    partners = [(x, y, z, other), (x, y1, z, c), (x, NY - 1 - y, z, c), (x1, y, z, c), (NX - 1 - x, y, z, c)]

    def c_move(s):
        return rcopy(csend.at[s], crecv.at[s], c_ss.at[s], c_rs.at[s], partners[s])

    def c_step(s):
        if s > 0:
            c_move(s - 1).wait()
            total = csend[s - 1] + crecv[s - 1]
        if s == len(partners):
            cnt_ref[...] = total[0:1]
            return
        if s > 0:
            csend[s] = total
        c_move(s).start()

    def weigh(b):
        same = keys[b][:, None, :] == slot_row
        placed = jnp.where(same, wks[b][:, None, :], 0.0).reshape(NS * PER * SLOTS, tok).T
        high = placed.astype(BF16)
        wh[b] = high
        wl[b] = (placed - high.astype(F32)).astype(BF16)

    @pl.loop(0, NC + 4)
    def _(i):
        guarded(i - 2, lambda k: z_hop(k, 4))
        guarded(i - 1, lambda k: z_hop(k, 3))
        guarded(i, lambda k: z_hop(k, 2))
        guarded(i + 2, lambda k: z_hop(k, 1))
        guarded(i - 3, pick_rows)
        guarded(i - 4, pass_rows)

        @pl.when(i == 3)
        def _():
            g_relay(0, 0)

        @pl.when(i == 5)
        def _():
            g_relay(1, 0)

        @pl.when(i == 6)
        def _():
            got(wdn.at[:, :, x], wdl_s)
            for u in range(early):
                d_own(u)
            g_own(0, 1)

        @pl.when(i == 10)
        def _():
            for u in range(early):
                d_relay(u)
            g_own(1, 1)

        guarded(i - 4, weigh)

        @pl.when(i == 4)
        def _():
            csend[0] = lax.fori_loop(0, NZ, count, jnp.zeros((8, tok), F32))

        for s, at in enumerate((5, 6, 8, 11)):

            @pl.when(i == at)
            def _(s=s):
                c_step(s)

    @pl.loop(0, NC)
    def _(k):
        got(rb.at[k, pl.ds(0, NS - 1)], y1_rs.at[k])

    sent(xb.at[:, pl.ds(0, NZ - 1)], z_ss)
    sent(sb.at[:, pl.ds(0, NS - 1)], y1_ss)
    sent(rl1, f1_ss)
    sent(mroute.at[pl.ds(0, NZ - 1)], meta_ss.at[0])
    sent(mweight.at[pl.ds(0, NZ - 1)], meta_ss.at[1])

    def hidden_of(j, xs):
        @pl.loop(0, 2)
        def _(t):
            part = pl.ds(t * (NS // 2), NS // 2)
            gate = up = None
            for k in range(NC):
                rows = rb[k, part, j].reshape(NS // 2 * SLOTS, width)
                cols = slice(k * width, (k + 1) * width)
                g = lax.dot_general(rows, wgu[0, j, xs, :, cols], NT, preferred_element_type=F32)
                u = lax.dot_general(rows, wgu[1, j, xs, :, cols], NT, preferred_element_type=F32)
                gate = g if gate is None else gate + g
                up = u if up is None else up + u
            act = (gate / (1.0 + jnp.exp(-gate)) * up).astype(BF16)
            half = NS // 2 * SLOTS
            hid[j, xs, pl.ds(pl.multiple_of(t * half, half), half), :] = act

    opposite = wrap(x + 2, NX)

    def g_relayed(j):
        for w in range(2):
            got(g_piece(w, j, opposite), g_rs.at[w, j, 1])

    g_relay(0, 1)
    g_relayed(0)

    @pl.loop(0, NX)
    def _(xs):
        hidden_of(0, xs)

    def second_expert():
        @pl.loop(0, NX - 1)
        def _(step):
            hidden_of(1, wrap(x + 3 + step, NX))

        d_relay(early)
        d_own(early + 1)
        d_own(early + 2)
        g_relayed(1)
        hidden_of(1, opposite)

    def down(u):
        k, j = unit(u)
        got(wdn.at[k, j, opposite], d_rs.at[u, 1])
        total = None
        for xs in range(NX):
            t = jnp.dot(hid[j, xs], wdn[k, j, xs], preferred_element_type=F32)
            total = t if total is None else total + t
        sb[k, :, j] = total.astype(BF16).reshape(NS, SLOTS, width)
        cb[k, mine, j] = sb[k, mine, j]
        y_send(
            lambda d: sb.at[k, d, j], lambda d: cb.at[k, d, j], lambda d: rl2.at[k, d, j],
            y2_ss, y2_rs.at[k, j], l2_rs.at[k, j],
        )

    def pass_back(u):
        k, j = unit(u)
        y_forward(
            lambda d: cb.at[k, d, j], lambda d: rl2.at[k, d, j], rl2.at[k, :, j],
            f2_ss, y2_rs.at[k, j], l2_rs.at[k, j],
        )

    def r_hop(k, h):
        s = 1 - 2 * lax.rem(k, 2)
        if h >= 2:
            got(rsb.at[k, :, h - 2], r_rs.at[k, h - 2])
        for way, t, step in ((0, z + (5 - h) * s, s), (1, z - (4 - h) * s, -s)):
            if h == 4 and way == 1:
                continue
            t = wrap(t, NZ)
            if h >= 2:
                xb[k, t] = (xb[k, t].astype(F32) + rsb[k, way, h - 2].astype(F32)).astype(BF16)
            to = (x, y, wrap(z + step, NZ), c)
            rcopy(xb.at[k, t], rsb.at[k, way, h - 1], r_ss, r_rs.at[k, h - 1], to).start()

    def combine(k):
        for j in range(PER):
            got(cb.at[k, pl.ds(0, NS - 1), j], y2_rs.at[k, j])

        @pl.loop(0, 2)
        def _(p):
            part = pl.ds(p * (NZ // 2), NZ // 2)
            served = cb[k].reshape(NS * PER * SLOTS, width)
            hi = wh[part].reshape(NZ // 2 * tok, NS * PER * SLOTS)
            lo = wl[part].reshape(NZ // 2 * tok, NS * PER * SLOTS)
            summed = jnp.dot(hi, served, preferred_element_type=F32)
            summed += jnp.dot(lo, served, preferred_element_type=F32)
            xb[k, part] = summed.astype(BF16).reshape(NZ // 2, tok, width)

        r_hop(k, 1)

    def out_copy(k):
        return pltpu.make_async_copy(outb.at[k], out_ref.at[:, columns(k)], out_s)

    def finish(k):
        got(rsb.at[k, 0, 3], r_rs.at[k, 3])
        value = xb[k, z].astype(F32) + rsb[k, 0, 3].astype(F32) + rsb[k, 1, 2].astype(F32)
        outb[k] = value.astype(BF16)
        out_copy(k).start()

    def completed(u, fn):
        k, j = unit(u)

        @pl.when(jnp.logical_and(jnp.logical_and(u >= early, u < units), j == 1))
        def _():
            fn(k)

    @pl.loop(0, units + 12)
    def _(i):
        guarded(i - 2, pass_back, 0, units)
        completed(i - 12, finish)
        completed(i - 10, lambda k: r_hop(k, 4))
        completed(i - 8, lambda k: r_hop(k, 3))
        completed(i - 6, lambda k: r_hop(k, 2))
        completed(i - 4, combine)

        @pl.when(i == early - 1)
        def _():
            d_own(early)
            g_relay(1, 1)

        @pl.when(i == early)
        def _():
            second_expert()

        guarded(i + 1, d_relay, early + 1, units)
        guarded(i + 3, d_own, early + 3, units)
        guarded(i, down, 0, units)

        @pl.when(i == early + 2)
        def _():
            c_step(4)

        @pl.when(i == units - 2)
        def _():
            c_step(5)

    sent(wgu.at[:, :, pl.ds(0, NX - 1)], g_ss)
    sent(wdn.at[:, :, pl.ds(0, NX - 1)], d_ss)
    sent(sb.at[:, pl.ds(0, NS - 1)], y2_ss)
    sent(rl2, f2_ss)
    sent(xb.at[:, pl.ds(0, NZ - 1)], r_ss)
    got(outb, out_s)


def close(mean_load, experts, mixed_ref, total_ref, bias_ref, out_ref, new_bias_ref, count_ref):
    out_ref[...] = mixed_ref[...]
    totals = total_ref[...]
    over = mean_load - experts * totals
    sign = jnp.where(over > 0.0, 1.0, jnp.where(over < 0.0, -1.0, 0.0))
    new_bias_ref[...] = bias_ref[...] + bias_rate * sign
    count_ref[...] = totals.astype(jnp.int32)


def body(tokens, routes, route_weight, bias, w_gate, w_up, w_down):
    tok, feat = tokens.shape
    per, ff, _ = w_gate.shape
    experts = bias.shape[0]
    width = feat // NC
    rows = NS * PER * SLOTS
    vmem, anywhere = pl.BlockSpec(memory_space=pltpu.VMEM), pl.BlockSpec(memory_space=pl.ANY)
    dma = pltpu.SemaphoreType.DMA
    mixed, totals = pl.pallas_call(
        kernel,
        out_shape=(
            jax.ShapeDtypeStruct((tok, feat), BF16),
            jax.ShapeDtypeStruct((1, experts), F32),
        ),
        in_specs=[vmem, vmem, anywhere, anywhere, anywhere, anywhere],
        out_specs=(anywhere, vmem),
        scratch_shapes=[
            pltpu.VMEM((NC, NZ, tok, width), BF16),
            pltpu.VMEM((rows, NZ * tok), BF16),
            pltpu.VMEM((NZ, tok, rows), BF16),
            pltpu.VMEM((NZ, tok, rows), BF16),
            pltpu.VMEM((NC, NS, PER, SLOTS, width), BF16),
            pltpu.VMEM((NC, NS, PER, SLOTS, width), BF16),
            pltpu.VMEM((NC, NS, PER, SLOTS, width), BF16),
            pltpu.VMEM((2, per, NX, ff, feat), BF16),
            pltpu.VMEM((NC, per, NX, ff, width), BF16),
            pltpu.VMEM((per, NX, NS * SLOTS, ff), BF16),
            pltpu.VMEM((NC, 2, PER, SLOTS, width), BF16),
            pltpu.VMEM((NC, 2, PER, SLOTS, width), BF16),
            pltpu.VMEM((NC, 2, 4, tok, width), BF16),
            pltpu.VMEM((NZ, 8, tok), jnp.int32),
            pltpu.VMEM((NZ, 8, tok), F32),
            pltpu.VMEM((NZ, NS * PER, tok), F32),
            pltpu.VMEM((NZ, NS * PER, tok), F32),
            pltpu.VMEM((5, 8, tok), F32),
            pltpu.VMEM((5, 8, tok), F32),
            pltpu.VMEM((NC, tok, width), BF16),
            dma((2,)),
            dma((2,)),
            dma,
            dma,
            dma((2,)),
            dma((2, 4)),
            dma((5,)),
            dma((5,)),
            dma,
            dma((NC, 4)),
            dma,
            dma((NC,)),
            dma((NC,)),
            dma,
            dma,
            dma((NC, PER)),
            dma((NC, PER)),
            dma,
            dma,
            dma((NC, 4)),
            dma,
            dma((2, PER, 2)),
            dma,
            dma((2 * NC, 2)),
        ],
        compiler_params=pltpu.CompilerParams(
            collective_id=0, has_side_effects=True, vmem_limit_bytes=67_043_328
        ),
        name="moe_layer",
    )(routes.T, route_weight.T, tokens, w_gate, w_up, w_down)
    everyone = NX * NY * NZ * NCORE
    mixed, new_bias, counts = pl.pallas_call(
        functools.partial(close, float(tok * routes.shape[1] * everyone), float(experts)),
        out_shape=(
            jax.ShapeDtypeStruct((tok, feat), BF16),
            jax.ShapeDtypeStruct((1, experts), F32),
            jax.ShapeDtypeStruct((1, experts), jnp.int32),
        ),
        in_specs=[vmem] * 3,
        out_specs=(vmem,) * 3,
        name="moe_close",
    )(mixed, totals, bias.reshape(1, experts))
    return mixed, new_bias.reshape(experts), counts.reshape(experts)


def solution(mesh):
    torus = Mesh(mesh.devices.reshape(NX, NY, NZ, NCORE), DP_EXPERT)
    placed = (
        P(DP_EXPERT, None),
        P(DP_EXPERT, None),
        P(DP_EXPERT, None),
        P(),
        P(EXPERT, "dp", None),
        P(EXPERT, "dp", None),
        P(EXPERT, "dp", None),
    )
    return jax.shard_map(
        body, mesh=torus, in_specs=placed, out_specs=(P(DP_EXPERT, None), P(), P()), check_vma=False
    )
```

```python
import functools

import jax
import jax.numpy as jnp
from jax import lax
from jax.experimental import pallas as pl
from jax.experimental.pallas import tpu as pltpu
from jax.sharding import Mesh
from jax.sharding import PartitionSpec as P

EXPERT = ("expert_0", "expert_1", "expert_2")
DP_EXPERT = ("dp", "expert_0", "expert_1", "expert_2")
MESH = pl.DeviceIdType.MESH
BF16, F32 = jnp.bfloat16, jnp.float32

NX, NY, NZ, NCORE = 4, 4, 8, 2
PER = 2
CAP = 10
NS = NY * NCORE
SLOTS = CAP * NZ
SPAN = 32
NC = 8
PARTS = 2
bias_rate = 0.05

NT = (((1,), (1,)), ((), ()))


def wrap(v, n):
    return lax.rem(v + 2 * n, n)


def kernel(
    route_ref, weight_ref, tok_ref, wg_ref, wu_ref, wd_ref,
    out_ref, cnt_ref,
    xb, pm, ws, sb, rb, cb, wgu, wdn, hid, rl1, rl2, rsb, mroute, mweight, keys, wks, csend, crecv, outb,
    loc_s, tok_s, wdl_s, out_s, meta_ss, meta_rs, c_ss, c_rs,
    z_ss, z_rs, y1_ss, y1_rs, l1_rs, f1_ss, y2_ss, y2_rs, l2_rs, f2_ss, r_ss, r_rs,
    g_ss, g_rs, d_ss, d_rs,
):
    x, y = lax.axis_index("dp"), lax.axis_index("expert_0")
    z, c = lax.axis_index("expert_1"), lax.axis_index("expert_2")
    feat = tok_ref.shape[1]
    width = feat // NC
    thin = width // PARTS
    tok = tok_ref.shape[0]
    ff = wg_ref.shape[1]
    xp, xm = wrap(x + 1, NX), wrap(x - 1, NX)
    yp, ym = wrap(y + 1, NY), wrap(y - 1, NY)
    other = 1 - c
    mine = y * NCORE + c
    home = (x, y, z, c)

    def rcopy(src, dst, ss, rs, to):
        return pltpu.make_async_remote_copy(
            src_ref=src, dst_ref=dst, send_sem=ss, recv_sem=rs, device_id=to, device_id_type=MESH
        )

    def got(ref, sem):
        rcopy(ref, ref, sem, sem, (xp, y, z, c)).wait_recv()

    def sent(ref, sem):
        rcopy(ref, ref, sem, sem, (xp, y, z, c)).wait_send()

    own_g = [
        pltpu.make_async_copy(wg_ref, wgu.at[0, :, x], loc_s.at[0]),
        pltpu.make_async_copy(wu_ref, wgu.at[1, :, x], loc_s.at[1]),
    ]
    own_g[0].start()
    own_g[1].start()

    def columns(k):
        return pl.ds(pl.multiple_of(k * width, width), width)

    def tok_copy(k):
        return pltpu.make_async_copy(tok_ref.at[:, columns(k)], xb.at[k, z], tok_s.at[(k + NC - 1) // NC])

    def wd_copy(k):
        return pltpu.make_async_copy(wd_ref.at[:, :, columns(k)], wdn.at[k, :, x], wdl_s)

    @pl.loop(0, NC)
    def _(k):
        tok_copy(k).start()

    @pl.loop(0, NC)
    def _(k):
        wd_copy(k).start()

    barrier = pltpu.get_barrier_semaphore()
    peers = [(xp, y, z, c), (xm, y, z, c), (x, y, z, other)]
    peers += [(x, yy, z, cc) for yy in (yp, ym) for cc in range(NCORE)]
    peers += [(x, y, wrap(z + 1, NZ), c), (x, y, wrap(z - 1, NZ), c)]
    for p in peers:
        pl.semaphore_signal(barrier, inc=1, device_id=p, device_id_type=MESH)
    pl.semaphore_wait(barrier, len(peers))

    def g_piece(w, j, xs):
        return wgu.at[w, j, xs]

    def g_own(w, j):
        a = g_piece(w, j, x)
        rcopy(a, a, g_ss, g_rs.at[w, j, 0], (xp, y, z, c)).start()
        rcopy(a, a, g_ss, g_rs.at[w, j, 0], (xm, y, z, c)).start()

    def g_arrived(w, j):
        got(wgu.at[w, :, x], g_rs.at[w, j, 0])

    def halves(ref):
        rows = ref.shape[0] // 2
        return ref.at[pl.ds(0, rows)], ref.at[pl.ds(rows, rows)]

    def g_relay(w, j):
        g_arrived(w, j)
        a = halves(g_piece(w, j, xm))[0]
        rcopy(a, a, g_ss, g_rs.at[w, j, 1], (xp, y, z, c)).start()
        b = halves(g_piece(w, j, xp))[1]
        rcopy(b, b, g_ss, g_rs.at[w, j, 1], (xm, y, z, c)).start()

    own_g[0].wait()
    g_own(0, 0)
    own_g[1].wait()
    g_own(1, 0)

    def z_hop(k, h):
        s = 1 - 2 * lax.rem(k, 2)
        far = xb.at[k, wrap(z - s * (h - 1), NZ)]
        near = xb.at[k, wrap(z + s * (h - 1), NZ)]
        if h >= 2:
            got(xb.at[k, pl.ds(0, 2)], z_rs.at[k, h - 2])
        rcopy(far, far, z_ss, z_rs.at[k, h - 1], (x, y, wrap(z + s, NZ), c)).start()
        if h < 4:
            rcopy(near, near, z_ss, z_rs.at[k, h - 1], (x, y, wrap(z - s, NZ), c)).start()

    def m_hop(h):
        for a, (own, held) in enumerate(((route_ref, mroute), (weight_ref, mweight))):
            if h >= 2:
                got(held.at[pl.ds(0, 2)], meta_rs.at[a, h - 2])
            p, q = wrap(z - (h - 1), NZ), wrap(z + (h - 1), NZ)
            rcopy(
                own if h == 1 else held.at[p], held.at[p], meta_ss.at[a], meta_rs.at[a, h - 1],
                (x, y, wrap(z + 1, NZ), c),
            ).start()
            if h < 4:
                rcopy(
                    own if h == 1 else held.at[q], held.at[q], meta_ss.at[a], meta_rs.at[a, h - 1],
                    (x, y, wrap(z - 1, NZ), c),
                ).start()

    m_hop(1)
    mroute[z] = route_ref[...]
    mweight[z] = weight_ref[...]
    tok_copy(0).wait()
    z_hop(0, 1)
    m_hop(2)
    m_hop(3)
    got(xb.at[pl.ds(0, NC - 1), z], tok_s.at[1])
    z_hop(1, 1)
    m_hop(4)

    got(mroute.at[0], meta_rs.at[0, 3])
    got(mweight.at[0], meta_rs.at[1, 3])
    row = lax.broadcasted_iota(jnp.int32, (NS * PER, tok), 0)
    expert = (row // 4) * (NZ * 4) + z * 4 + row % 4
    before = (
        lax.broadcasted_iota(jnp.int32, (tok, tok), 0)
        < lax.broadcasted_iota(jnp.int32, (tok, tok), 1)
    ).astype(F32).astype(BF16)
    slot_row = lax.broadcasted_iota(jnp.int32, (NS * PER, SLOTS, tok), 1).astype(F32)

    @pl.loop(0, NZ)
    def _(b):
        hit = jnp.zeros((NS * PER, tok), F32)
        weight = jnp.zeros((NS * PER, tok), F32)
        for k in range(8):
            same = mroute[b, k : k + 1, :] == expert
            hit = jnp.where(same, 1.0, hit)
            weight = jnp.where(same, mweight[b, k : k + 1, :], weight)
        rank = jnp.dot(hit.astype(BF16), before, preferred_element_type=F32)
        key = jnp.where(jnp.logical_and(hit > 0.0, rank < CAP), b.astype(F32) * CAP + rank, -1.0)
        keys[b] = key
        wks[b] = weight
        pick = jnp.where(key[:, None, :] == slot_row, 1.0, 0.0)
        at = pl.ds(pl.multiple_of(b * tok, tok), tok)
        pm[:, at] = pick.reshape(NS * PER * SLOTS, tok).astype(BF16)

    def y_far(src, rl, ss, ls):
        opp = wrap(y + 2, NY)
        for cc, yf in ((0, yp), (1, ym)):
            rcopy(src(opp * NCORE + cc), rl(cc), ss, ls, (x, yf, z, c)).start()

    def y_send(src, dst, ss, rs):
        rcopy(src(y * NCORE + other), dst(mine), ss, rs, (x, y, z, other)).start()
        for yy in (yp, ym):
            for cc in range(NCORE):
                rcopy(src(yy * NCORE + cc), dst(mine), ss, rs, (x, yy, z, cc)).start()

    def y_forward(dst, rl, fs, rs):
        rcopy(rl(0), dst(ym * NCORE + c), fs, rs, (x, yp, z, 0)).start()
        rcopy(rl(1), dst(yp * NCORE + c), fs, rs, (x, ym, z, 1)).start()

    def pick_rows(k):
        got(xb.at[k, 0], z_rs.at[k, 3])
        half = NS * PER * SLOTS // 2

        @pl.loop(0, 2)
        def _(p):
            rows = pm[pl.ds(pl.multiple_of(p * half, half), half), :]
            picked = jnp.dot(rows, xb[k].reshape(NZ * tok, width), preferred_element_type=F32)
            picked = picked.astype(BF16).reshape(NS // 2, PER, SLOTS, width)
            sb[k, pl.ds(p * (NS // 2), NS // 2)] = picked

        rb[k, mine] = sb[k, mine]
        y_far(lambda d: sb.at[k, d], lambda d: rl1.at[k, d], y1_ss, l1_rs.at[k])
        y_send(lambda d: sb.at[k, d], lambda d: rb.at[k, d], y1_ss, y1_rs.at[k])

    def pass_rows(k):
        got(rl1.at[k], l1_rs.at[k])
        y_forward(lambda d: rb.at[k, d], lambda d: rl1.at[k, d], f1_ss, y1_rs.at[k])

    def guarded(k, fn, first=0, last=NC):
        @pl.when(jnp.logical_and(k >= first, k < last))
        def _():
            fn(k)

    def d_own(k, j):
        a = wdn.at[k, j, x]
        rcopy(a, a, d_ss, d_rs.at[k, j, 0], (xp, y, z, c)).start()
        rcopy(a, a, d_ss, d_rs.at[k, j, 0], (xm, y, z, c)).start()

    def d_relay(k, j):
        got(wdn.at[k, :, x], d_rs.at[k, j, 0])
        a = halves(wdn.at[k, j, xm])[0]
        rcopy(a, a, d_ss, d_rs.at[k, j, 1], (xp, y, z, c)).start()
        b = halves(wdn.at[k, j, xp])[1]
        rcopy(b, b, d_ss, d_rs.at[k, j, 1], (xm, y, z, c)).start()

    expert_row = lax.broadcasted_iota(jnp.int32, (tok, tok), 0)

    def count(b, total):
        hit = jnp.zeros((tok, tok), F32)
        for k in range(8):
            hit = jnp.where(mroute[b, k : k + 1, :] == expert_row, 1.0, hit)
        ones = jnp.ones((8, tok), BF16)
        return total + lax.dot_general(ones, hit.astype(BF16), NT, preferred_element_type=F32)

    y1 = y + 1 - 2 * lax.rem(y, 2)
    x1 = x + 1 - 2 * lax.rem(x, 2)
    partners = [(x, y, z, other), (x, y1, z, c), (x, NY - 1 - y, z, c), (x1, y, z, c), (NX - 1 - x, y, z, c)]

    def c_move(s):
        return rcopy(csend.at[s], crecv.at[s], c_ss.at[s], c_rs.at[s], partners[s])

    def c_step(s):
        if s > 0:
            c_move(s - 1).wait()
            total = csend[s - 1] + crecv[s - 1]
        if s == len(partners):
            cnt_ref[...] = total[0:1]
            return
        if s > 0:
            csend[s] = total
        c_move(s).start()

    span_row = lax.broadcasted_iota(jnp.int32, (NS * PER, SPAN, tok), 1)

    def weigh(b):
        pair = b // 2
        same = keys[b][:, None, :] == (span_row + 16 * pair).astype(F32)
        placed = jnp.where(same, wks[b][:, None, :], 0.0).reshape(NS * PER * SPAN, tok).T
        high = placed.astype(BF16)
        ws[pair, 0, b % 2] = high
        ws[pair, 1, b % 2] = (placed - high.astype(F32)).astype(BF16)

    @pl.loop(0, NC + 4)
    def _(i):
        guarded(i - 2, lambda k: z_hop(k, 4))
        guarded(i - 1, lambda k: z_hop(k, 3))
        guarded(i, lambda k: z_hop(k, 2))
        guarded(i + 2, lambda k: z_hop(k, 1))
        guarded(i - 3, pick_rows)
        guarded(i - 4, pass_rows)

        @pl.when(i == 3)
        def _():
            g_relay(0, 0)

        @pl.when(i == 5)
        def _():
            g_relay(1, 0)
            g_own(0, 1)
            g_own(1, 1)

        @pl.when(i == 10)
        def _():
            g_relay(0, 1)

        guarded(i - 4, weigh)

        @pl.when(i == 4)
        def _():
            csend[0] = lax.fori_loop(0, NZ, count, jnp.zeros((8, tok), F32))

        for s, at in enumerate((5, 6, 8, 11)):

            @pl.when(i == at)
            def _(s=s):
                c_step(s)

    @pl.loop(0, NC)
    def _(k):
        got(rb.at[k, pl.ds(0, NS - 1)], y1_rs.at[k])

    sent(xb.at[:, pl.ds(0, NZ - 1)], z_ss)
    sent(sb.at[:, pl.ds(0, NS - 1)], y1_ss)
    sent(rl1, f1_ss)
    sent(mroute.at[pl.ds(0, NZ - 1)], meta_ss.at[0])
    sent(mweight.at[pl.ds(0, NZ - 1)], meta_ss.at[1])

    def hidden_of(j, xs):
        @pl.loop(0, 2)
        def _(t):
            part = pl.ds(t * (NS // 2), NS // 2)
            gate = up = None
            for k in range(NC):
                rows = rb[k, part, j].reshape(NS // 2 * SLOTS, width)
                cols = slice(k * width, (k + 1) * width)
                g = lax.dot_general(rows, wgu[0, j, xs, :, cols], NT, preferred_element_type=F32)
                u = lax.dot_general(rows, wgu[1, j, xs, :, cols], NT, preferred_element_type=F32)
                gate = g if gate is None else gate + g
                up = u if up is None else up + u
            act = (gate / (1.0 + jnp.exp(-gate)) * up).astype(BF16)
            half = NS // 2 * SLOTS
            hid[j, xs, pl.ds(pl.multiple_of(t * half, half), half), :] = act

    opposite = wrap(x + 2, NX)

    def g_relayed(j):
        for w in range(2):
            got(g_piece(w, j, opposite), g_rs.at[w, j, 1])

    got(wdn.at[:, :, x], wdl_s)
    d_own(0, 0)
    g_relay(1, 1)
    g_relayed(0)

    @pl.loop(0, NX)
    def _(xs):
        hidden_of(0, xs)

    @pl.loop(0, NX - 1)
    def _(step):
        hidden_of(1, wrap(x + 3 + step, NX))

    d_relay(0, 0)
    d_own(0, 1)
    d_own(1, 0)
    g_relayed(1)
    hidden_of(1, opposite)

    def down(k, j):
        got(wdn.at[k, j, opposite], d_rs.at[k, j, 1])
        total = None
        for xs in range(NX):
            t = jnp.dot(hid[j, xs], wdn[k, j, xs], preferred_element_type=F32)
            total = t if total is None else total + t
        sb[k, :, j] = total.astype(BF16).reshape(NS, SLOTS, width)
        cb[k, mine, j] = sb[k, mine, j]
        for q in range(PARTS):
            y_far(
                lambda d: sb.at[k, d, j, :, part(q)], lambda d: rl2.at[k, d, j, :, part(q)],
                y2_ss, l2_rs.at[k, j],
            )
        for q in range(PARTS):
            y_send(
                lambda d: sb.at[k, d, j, :, part(q)], lambda d: cb.at[k, d, j, :, part(q)],
                y2_ss, y2_rs.at[k, q],
            )

    def part(q):
        return pl.ds(q * thin, thin)

    def pass_back(k, j):
        got(rl2.at[k, :, j], l2_rs.at[k, j])
        for q in range(PARTS):
            y_forward(
                lambda d: cb.at[k, d, j, :, part(q)], lambda d: rl2.at[k, d, j, :, part(q)],
                f2_ss, y2_rs.at[k, q],
            )

    along = [wrap(z + o, NZ) for o in range(NZ)]

    def r_hop(k, q, h):
        s = 1 - 2 * q
        cols = part(q)
        if h >= 2:
            got(rsb.at[k, :, h - 2, :, cols], r_rs.at[k, q, h - 2])
        for way, t, step in ((0, (5 - h) * s, s), (1, (h - 4) * s, -s)):
            if h == 4 and way == 1:
                continue
            t = along[t % NZ]
            if h >= 2:
                held = xb[k, t, :, cols].astype(F32) + rsb[k, way, h - 2, :, cols].astype(F32)
                xb[k, t, :, cols] = held.astype(BF16)
            to = (x, y, along[step % NZ], c)
            rcopy(
                xb.at[k, t, :, cols], rsb.at[k, way, h - 1, :, cols], r_ss, r_rs.at[k, q, h - 1], to
            ).start()

    def combine(k, q):
        got(cb.at[k, pl.ds(0, NS - 1), :, :, part(q)], y2_rs.at[k, q])
        for pair in range(NZ // 2):
            served = cb[k, :, :, 16 * pair : 16 * pair + SPAN, part(q)].reshape(NS * PER * SPAN, thin)
            rows = ws[pair].reshape(4 * tok, NS * PER * SPAN)
            summed = jnp.dot(rows, served, preferred_element_type=F32)
            summed = summed[: 2 * tok] + summed[2 * tok :]
            xb[k, 2 * pair : 2 * pair + 2, :, part(q)] = summed.astype(BF16).reshape(2, tok, thin)
        r_hop(k, q, 1)

    def out_copy(k, q):
        at = pl.ds(pl.multiple_of(k * width + q * thin, thin), thin)
        return pltpu.make_async_copy(outb.at[k, :, part(q)], out_ref.at[:, at], out_s)

    def finish(k, q):
        cols = part(q)
        got(rsb.at[k, 0, 3, :, cols], r_rs.at[k, q, 3])
        value = xb[k, z, :, cols].astype(F32) + rsb[k, 0, 3, :, cols].astype(F32)
        value += rsb[k, 1, 2, :, cols].astype(F32)
        outb[k, :, cols] = value.astype(BF16)
        out_copy(k, q).start()

    @pl.loop(0, NC + 5)
    def _(i):
        guarded(i - 1, lambda k: pass_back(k, 0))
        guarded(i - 3, lambda k: r_hop(k, 0, 2))
        guarded(i - 4, lambda k: r_hop(k, 1, 3))
        guarded(i, lambda k: d_relay(k, 1))
        guarded(i + 1, lambda k: d_own(k, 1), 1)
        guarded(i, lambda k: down(k, 0))
        guarded(i - 2, lambda k: combine(k, 0))
        guarded(i - 5, lambda k: finish(k, 0))
        guarded(i - 3, lambda k: r_hop(k, 1, 2))

        guarded(i - 1, lambda k: pass_back(k, 1))
        guarded(i - 2, lambda k: combine(k, 1))
        guarded(i - 4, lambda k: r_hop(k, 0, 4))
        guarded(i - 5, lambda k: finish(k, 1))
        guarded(i + 1, lambda k: d_relay(k, 0), 1)
        guarded(i + 2, lambda k: d_own(k, 0), 2)
        guarded(i, lambda k: down(k, 1))
        guarded(i - 3, lambda k: r_hop(k, 0, 3))
        guarded(i - 4, lambda k: r_hop(k, 1, 4))

        @pl.when(i == 2)
        def _():
            c_step(4)

        @pl.when(i == NC - 1)
        def _():
            c_step(5)

    sent(wgu.at[:, :, pl.ds(0, NX - 1)], g_ss)
    sent(wdn.at[:, :, pl.ds(0, NX - 1)], d_ss)
    sent(sb.at[:, pl.ds(0, NS - 1)], y2_ss)
    sent(rl2, f2_ss)
    sent(xb.at[:, pl.ds(0, NZ - 1)], r_ss)
    got(outb, out_s)


def close(mean_load, experts, mixed_ref, total_ref, bias_ref, out_ref, new_bias_ref, count_ref):
    out_ref[...] = mixed_ref[...]
    totals = total_ref[...]
    over = mean_load - experts * totals
    sign = jnp.where(over > 0.0, 1.0, jnp.where(over < 0.0, -1.0, 0.0))
    new_bias_ref[...] = bias_ref[...] + bias_rate * sign
    count_ref[...] = totals.astype(jnp.int32)


def body(tokens, routes, route_weight, bias, w_gate, w_up, w_down):
    tok, feat = tokens.shape
    per, ff, _ = w_gate.shape
    experts = bias.shape[0]
    width = feat // NC
    rows = NS * PER * SLOTS
    vmem, anywhere = pl.BlockSpec(memory_space=pltpu.VMEM), pl.BlockSpec(memory_space=pl.ANY)
    dma = pltpu.SemaphoreType.DMA
    mixed, totals = pl.pallas_call(
        kernel,
        out_shape=(
            jax.ShapeDtypeStruct((tok, feat), BF16),
            jax.ShapeDtypeStruct((1, experts), F32),
        ),
        in_specs=[vmem, vmem, anywhere, anywhere, anywhere, anywhere],
        out_specs=(anywhere, vmem),
        scratch_shapes=[
            pltpu.VMEM((NC, NZ, tok, width), BF16),
            pltpu.VMEM((rows, NZ * tok), BF16),
            pltpu.VMEM((NZ // 2, 2, 2, tok, NS * PER * SPAN), BF16),
            pltpu.VMEM((NC, NS, PER, SLOTS, width), BF16),
            pltpu.VMEM((NC, NS, PER, SLOTS, width), BF16),
            pltpu.VMEM((NC, NS, PER, SLOTS, width), BF16),
            pltpu.VMEM((2, per, NX, ff, feat), BF16),
            pltpu.VMEM((NC, per, NX, ff, width), BF16),
            pltpu.VMEM((per, NX, NS * SLOTS, ff), BF16),
            pltpu.VMEM((NC, 2, PER, SLOTS, width), BF16),
            pltpu.VMEM((NC, 2, PER, SLOTS, width), BF16),
            pltpu.VMEM((NC, 2, 4, tok, width), BF16),
            pltpu.VMEM((NZ, 8, tok), jnp.int32),
            pltpu.VMEM((NZ, 8, tok), F32),
            pltpu.VMEM((NZ, NS * PER, tok), F32),
            pltpu.VMEM((NZ, NS * PER, tok), F32),
            pltpu.VMEM((5, 8, tok), F32),
            pltpu.VMEM((5, 8, tok), F32),
            pltpu.VMEM((NC, tok, width), BF16),
            dma((2,)),
            dma((2,)),
            dma,
            dma,
            dma((2,)),
            dma((2, 4)),
            dma((5,)),
            dma((5,)),
            dma,
            dma((NC, 4)),
            dma,
            dma((NC,)),
            dma((NC,)),
            dma,
            dma,
            dma((NC, PARTS)),
            dma((NC, PER)),
            dma,
            dma,
            dma((NC, PARTS, 4)),
            dma,
            dma((2, PER, 2)),
            dma,
            dma((NC, PER, 2)),
        ],
        compiler_params=pltpu.CompilerParams(
            collective_id=0, has_side_effects=True, vmem_limit_bytes=67_043_328
        ),
        name="moe_layer",
    )(routes.T, route_weight.T, tokens, w_gate, w_up, w_down)
    everyone = NX * NY * NZ * NCORE
    mixed, new_bias, counts = pl.pallas_call(
        functools.partial(close, float(tok * routes.shape[1] * everyone), float(experts)),
        out_shape=(
            jax.ShapeDtypeStruct((tok, feat), BF16),
            jax.ShapeDtypeStruct((1, experts), F32),
            jax.ShapeDtypeStruct((1, experts), jnp.int32),
        ),
        in_specs=[vmem] * 3,
        out_specs=(vmem,) * 3,
        name="moe_close",
    )(mixed, totals, bias.reshape(1, experts))
    return mixed, new_bias.reshape(experts), counts.reshape(experts)


def solution(mesh):
    torus = Mesh(mesh.devices.reshape(NX, NY, NZ, NCORE), DP_EXPERT)
    placed = (
        P(DP_EXPERT, None),
        P(DP_EXPERT, None),
        P(DP_EXPERT, None),
        P(),
        P(EXPERT, "dp", None),
        P(EXPERT, "dp", None),
        P(EXPERT, "dp", None),
    )
    return jax.shard_map(
        body, mesh=torus, in_specs=placed, out_specs=(P(DP_EXPERT, None), P(), P()), check_vma=False
    )
```

```python
import functools

import jax
import jax.numpy as jnp
from jax import lax
from jax.experimental import pallas as pl
from jax.experimental.pallas import tpu as pltpu
from jax.sharding import Mesh
from jax.sharding import PartitionSpec as P

EXPERT = ("expert_0", "expert_1", "expert_2")
DP_EXPERT = ("dp", "expert_0", "expert_1", "expert_2")
MESH = pl.DeviceIdType.MESH
BF16, F32 = jnp.bfloat16, jnp.float32

NX, NY, NZ, NCORE = 4, 4, 8, 2
PER = 2
CAP = 10
NS = NY * NCORE
SLOTS = CAP * NZ
SPAN = 32
NC = 8
PARTS = 2
bias_rate = 0.05

NT = (((1,), (1,)), ((), ()))


def wrap(v, n):
    return lax.rem(v + 2 * n, n)


def kernel(
    route_ref, weight_ref, tok_ref, wg_ref, wu_ref, wd_ref,
    out_ref, cnt_ref,
    xb, pm, ws, sb, rb, cb, wgu, wdn, hid, rl1, rl2, rsb, mroute, mweight, keys, wks, csend, crecv, ctotal, outb,
    loc_s, tok_s, wdl_s, out_s, tot_s, meta_ss, meta_rs, c_ss, c_rs,
    z_ss, z_rs, y1_ss, y1_rs, l1_rs, f1_ss, y2_ss, y2_rs, l2_rs, f2_ss, r_ss, r_rs,
    g_ss, g_rs, d_ss, d_rs,
):
    x, y = lax.axis_index("dp"), lax.axis_index("expert_0")
    z, c = lax.axis_index("expert_1"), lax.axis_index("expert_2")
    feat = tok_ref.shape[1]
    width = feat // NC
    thin = width // PARTS
    tok = tok_ref.shape[0]
    ff = wg_ref.shape[1]
    xp, xm = wrap(x + 1, NX), wrap(x - 1, NX)
    yp, ym = wrap(y + 1, NY), wrap(y - 1, NY)
    other = 1 - c
    mine = y * NCORE + c
    home = (x, y, z, c)

    def rcopy(src, dst, ss, rs, to):
        return pltpu.make_async_remote_copy(
            src_ref=src, dst_ref=dst, send_sem=ss, recv_sem=rs, device_id=to, device_id_type=MESH
        )

    def got(ref, sem):
        rcopy(ref, ref, sem, sem, (xp, y, z, c)).wait_recv()

    def sent(ref, sem):
        rcopy(ref, ref, sem, sem, (xp, y, z, c)).wait_send()

    own_g = [
        pltpu.make_async_copy(wg_ref, wgu.at[0, :, x], loc_s.at[0]),
        pltpu.make_async_copy(wu_ref, wgu.at[1, :, x], loc_s.at[1]),
    ]
    own_m = [
        pltpu.make_async_copy(route_ref, mroute.at[z], loc_s.at[2]),
        pltpu.make_async_copy(weight_ref, mweight.at[z], loc_s.at[3]),
    ]
    own_m[0].start()
    own_m[1].start()
    own_g[0].start()
    own_g[1].start()

    def columns(k):
        return pl.ds(pl.multiple_of(k * width, width), width)

    def tok_copy(k):
        return pltpu.make_async_copy(tok_ref.at[:, columns(k)], xb.at[k, z], tok_s.at[(k + NC - 1) // NC])

    def wd_copy(k):
        return pltpu.make_async_copy(wd_ref.at[:, :, columns(k)], wdn.at[k, :, x], wdl_s)

    @pl.loop(0, NC)
    def _(k):
        tok_copy(k).start()

    @pl.loop(0, NC)
    def _(k):
        wd_copy(k).start()

    barrier = pltpu.get_barrier_semaphore()
    peers = [(xp, y, z, c), (xm, y, z, c), (x, y, z, other)]
    peers += [(x, yy, z, cc) for yy in (yp, ym) for cc in range(NCORE)]
    peers += [(x, y, wrap(z + 1, NZ), c), (x, y, wrap(z - 1, NZ), c)]
    for p in peers:
        pl.semaphore_signal(barrier, inc=1, device_id=p, device_id_type=MESH)
    pl.semaphore_wait(barrier, len(peers))

    def g_piece(w, j, xs):
        return wgu.at[w, j, xs]

    def g_own(w, j):
        a = g_piece(w, j, x)
        rcopy(a, a, g_ss, g_rs.at[w, j, 0], (xp, y, z, c)).start()
        rcopy(a, a, g_ss, g_rs.at[w, j, 0], (xm, y, z, c)).start()

    def g_arrived(w, j):
        got(wgu.at[w, :, x], g_rs.at[w, j, 0])

    def halves(ref):
        rows = ref.shape[0] // 2
        return ref.at[pl.ds(0, rows)], ref.at[pl.ds(rows, rows)]

    def g_relay(w, j):
        g_arrived(w, j)
        a = halves(g_piece(w, j, xm))[0]
        rcopy(a, a, g_ss, g_rs.at[w, j, 1], (xp, y, z, c)).start()
        b = halves(g_piece(w, j, xp))[1]
        rcopy(b, b, g_ss, g_rs.at[w, j, 1], (xm, y, z, c)).start()

    own_g[0].wait()
    g_own(0, 0)
    own_g[1].wait()
    g_own(1, 0)

    def z_hop(k, h):
        s = 1 - 2 * lax.rem(k, 2)
        far = xb.at[k, wrap(z - s * (h - 1), NZ)]
        near = xb.at[k, wrap(z + s * (h - 1), NZ)]
        if h >= 2:
            got(xb.at[k, pl.ds(0, 2)], z_rs.at[k, h - 2])
        rcopy(far, far, z_ss, z_rs.at[k, h - 1], (x, y, wrap(z + s, NZ), c)).start()
        if h < 4:
            rcopy(near, near, z_ss, z_rs.at[k, h - 1], (x, y, wrap(z - s, NZ), c)).start()

    def m_hop(h):
        for a, held in enumerate((mroute, mweight)):
            if h >= 2:
                got(held.at[pl.ds(0, 2)], meta_rs.at[a, h - 2])
            p, q = wrap(z - (h - 1), NZ), wrap(z + (h - 1), NZ)
            rcopy(
                held.at[p], held.at[p], meta_ss.at[a], meta_rs.at[a, h - 1],
                (x, y, wrap(z + 1, NZ), c),
            ).start()
            if h < 4:
                rcopy(
                    held.at[q], held.at[q], meta_ss.at[a], meta_rs.at[a, h - 1],
                    (x, y, wrap(z - 1, NZ), c),
                ).start()

    own_m[0].wait()
    own_m[1].wait()
    m_hop(1)
    tok_copy(0).wait()
    z_hop(0, 1)
    m_hop(2)
    m_hop(3)
    got(xb.at[pl.ds(0, NC - 1), z], tok_s.at[1])
    z_hop(1, 1)
    m_hop(4)

    got(mroute.at[0], meta_rs.at[0, 3])
    got(mweight.at[0], meta_rs.at[1, 3])
    row = lax.broadcasted_iota(jnp.int32, (NS * PER, tok), 0)
    expert = (row // 4) * (NZ * 4) + z * 4 + row % 4
    before = (
        lax.broadcasted_iota(jnp.int32, (tok, tok), 0)
        < lax.broadcasted_iota(jnp.int32, (tok, tok), 1)
    ).astype(F32).astype(BF16)
    slot_row = lax.broadcasted_iota(jnp.int32, (NS * PER, SLOTS, tok), 1).astype(F32)

    @pl.loop(0, NZ)
    def _(b):
        hit = jnp.zeros((NS * PER, tok), F32)
        weight = jnp.zeros((NS * PER, tok), F32)
        for k in range(8):
            same = mroute[b, k : k + 1, :] == expert
            hit = jnp.where(same, 1.0, hit)
            weight = jnp.where(same, mweight[b, k : k + 1, :], weight)
        rank = jnp.dot(hit.astype(BF16), before, preferred_element_type=F32)
        key = jnp.where(jnp.logical_and(hit > 0.0, rank < CAP), b.astype(F32) * CAP + rank, -1.0)
        keys[b] = key
        wks[b] = weight
        pick = jnp.where(key[:, None, :] == slot_row, 1.0, 0.0)
        at = pl.ds(pl.multiple_of(b * tok, tok), tok)
        pm[:, at] = pick.reshape(NS * PER * SLOTS, tok).astype(BF16)

    def y_far(src, rl, ss, ls):
        opp = wrap(y + 2, NY)
        for cc, yf in ((0, yp), (1, ym)):
            rcopy(src(opp * NCORE + cc), rl(cc), ss, ls, (x, yf, z, c)).start()

    def y_send(src, dst, ss, rs):
        rcopy(src(y * NCORE + other), dst(mine), ss, rs, (x, y, z, other)).start()
        for yy in (yp, ym):
            for cc in range(NCORE):
                rcopy(src(yy * NCORE + cc), dst(mine), ss, rs, (x, yy, z, cc)).start()

    def y_forward(dst, rl, fs, rs):
        rcopy(rl(0), dst(ym * NCORE + c), fs, rs, (x, yp, z, 0)).start()
        rcopy(rl(1), dst(yp * NCORE + c), fs, rs, (x, ym, z, 1)).start()

    def pick_rows(k):
        got(xb.at[k, 0], z_rs.at[k, 3])
        half = NS * PER * SLOTS // 2

        @pl.loop(0, 2)
        def _(p):
            rows = pm[pl.ds(pl.multiple_of(p * half, half), half), :]
            picked = jnp.dot(rows, xb[k].reshape(NZ * tok, width), preferred_element_type=F32)
            picked = picked.astype(BF16).reshape(NS // 2, PER, SLOTS, width)
            sb[k, pl.ds(p * (NS // 2), NS // 2)] = picked

        rb[k, mine] = sb[k, mine]
        y_far(lambda d: sb.at[k, d], lambda d: rl1.at[k, d], y1_ss, l1_rs.at[k])
        y_send(lambda d: sb.at[k, d], lambda d: rb.at[k, d], y1_ss, y1_rs.at[k])

    def pass_rows(k):
        got(rl1.at[k], l1_rs.at[k])
        y_forward(lambda d: rb.at[k, d], lambda d: rl1.at[k, d], f1_ss, y1_rs.at[k])

    def guarded(k, fn, first=0, last=NC):
        @pl.when(jnp.logical_and(k >= first, k < last))
        def _():
            fn(k)

    def d_own(k, j):
        a = wdn.at[k, j, x]
        rcopy(a, a, d_ss, d_rs.at[k, j, 0], (xp, y, z, c)).start()
        rcopy(a, a, d_ss, d_rs.at[k, j, 0], (xm, y, z, c)).start()

    def d_relay(k, j):
        got(wdn.at[k, :, x], d_rs.at[k, j, 0])
        a = halves(wdn.at[k, j, xm])[0]
        rcopy(a, a, d_ss, d_rs.at[k, j, 1], (xp, y, z, c)).start()
        b = halves(wdn.at[k, j, xp])[1]
        rcopy(b, b, d_ss, d_rs.at[k, j, 1], (xm, y, z, c)).start()

    expert_row = lax.broadcasted_iota(jnp.int32, (tok, tok), 0)

    def count(b, total):
        hit = jnp.zeros((tok, tok), F32)
        for k in range(8):
            hit = jnp.where(mroute[b, k : k + 1, :] == expert_row, 1.0, hit)
        ones = jnp.ones((8, tok), BF16)
        return total + lax.dot_general(ones, hit.astype(BF16), NT, preferred_element_type=F32)

    y1 = y + 1 - 2 * lax.rem(y, 2)
    x1 = x + 1 - 2 * lax.rem(x, 2)
    partners = [(x, y, z, other), (x, y1, z, c), (x, NY - 1 - y, z, c), (x1, y, z, c), (NX - 1 - x, y, z, c)]

    def c_move(s):
        return rcopy(csend.at[s], crecv.at[s], c_ss.at[s], c_rs.at[s], partners[s])

    def c_step(s):
        if s > 0:
            c_move(s - 1).wait()
            total = csend[s - 1] + crecv[s - 1]
        if s == len(partners):
            ctotal[...] = total
            return
        if s > 0:
            csend[s] = total
        c_move(s).start()

    span_row = lax.broadcasted_iota(jnp.int32, (NS * PER, SPAN, tok), 1)

    def weigh(b):
        pair = b // 2
        same = keys[b][:, None, :] == (span_row + 16 * pair).astype(F32)
        placed = jnp.where(same, wks[b][:, None, :], 0.0).reshape(NS * PER * SPAN, tok).T
        high = placed.astype(BF16)
        ws[pair, 0, b % 2] = high
        ws[pair, 1, b % 2] = (placed - high.astype(F32)).astype(BF16)

    @pl.loop(0, NC + 4)
    def _(i):
        guarded(i - 2, lambda k: z_hop(k, 4))
        guarded(i - 1, lambda k: z_hop(k, 3))
        guarded(i, lambda k: z_hop(k, 2))
        guarded(i + 2, lambda k: z_hop(k, 1))
        guarded(i - 3, pick_rows)
        guarded(i - 4, pass_rows)

        @pl.when(i == 3)
        def _():
            g_relay(0, 0)

        @pl.when(i == 5)
        def _():
            g_relay(1, 0)
            g_own(0, 1)
            g_own(1, 1)

        @pl.when(i == 10)
        def _():
            g_relay(0, 1)

        guarded(i - 4, weigh)

        @pl.when(i == 4)
        def _():
            csend[0] = lax.fori_loop(0, NZ, count, jnp.zeros((8, tok), F32))

        for s, at in enumerate((5, 6, 8, 11)):

            @pl.when(i == at)
            def _(s=s):
                c_step(s)

    @pl.loop(0, NC)
    def _(k):
        got(rb.at[k, pl.ds(0, NS - 1)], y1_rs.at[k])

    sent(xb.at[:, pl.ds(0, NZ - 1)], z_ss)
    sent(sb.at[:, pl.ds(0, NS - 1)], y1_ss)
    sent(rl1, f1_ss)
    sent(mroute.at[pl.ds(0, NZ - 1)], meta_ss.at[0])
    sent(mweight.at[pl.ds(0, NZ - 1)], meta_ss.at[1])

    def hidden_of(j, xs):
        @pl.loop(0, 2)
        def _(t):
            part = pl.ds(t * (NS // 2), NS // 2)
            gate = up = None
            for k in range(NC):
                rows = rb[k, part, j].reshape(NS // 2 * SLOTS, width)
                cols = slice(k * width, (k + 1) * width)
                g = lax.dot_general(rows, wgu[0, j, xs, :, cols], NT, preferred_element_type=F32)
                u = lax.dot_general(rows, wgu[1, j, xs, :, cols], NT, preferred_element_type=F32)
                gate = g if gate is None else gate + g
                up = u if up is None else up + u
            act = (gate / (1.0 + jnp.exp(-gate)) * up).astype(BF16)
            half = NS // 2 * SLOTS
            hid[j, xs, pl.ds(pl.multiple_of(t * half, half), half), :] = act

    opposite = wrap(x + 2, NX)

    def g_relayed(j):
        for w in range(2):
            got(g_piece(w, j, opposite), g_rs.at[w, j, 1])

    got(wdn.at[:, :, x], wdl_s)
    d_own(0, 0)
    g_relay(1, 1)
    g_relayed(0)

    @pl.loop(0, NX)
    def _(xs):
        hidden_of(0, xs)

    @pl.loop(0, NX - 1)
    def _(step):
        hidden_of(1, wrap(x + 3 + step, NX))

    d_relay(0, 0)
    d_own(0, 1)
    d_own(1, 0)
    g_relayed(1)
    hidden_of(1, opposite)

    def down(k, j):
        got(wdn.at[k, j, opposite], d_rs.at[k, j, 1])
        total = None
        for xs in range(NX):
            t = jnp.dot(hid[j, xs], wdn[k, j, xs], preferred_element_type=F32)
            total = t if total is None else total + t
        sb[k, :, j] = total.astype(BF16).reshape(NS, SLOTS, width)
        cb[k, mine, j] = sb[k, mine, j]
        for q in range(PARTS):
            y_far(
                lambda d: sb.at[k, d, j, :, part(q)], lambda d: rl2.at[k, d, j, :, part(q)],
                y2_ss, l2_rs.at[k, j],
            )
        for q in range(PARTS):
            y_send(
                lambda d: sb.at[k, d, j, :, part(q)], lambda d: cb.at[k, d, j, :, part(q)],
                y2_ss, y2_rs.at[k, q],
            )

    def part(q):
        return pl.ds(q * thin, thin)

    def pass_back(k, j):
        got(rl2.at[k, :, j], l2_rs.at[k, j])
        for q in range(PARTS):
            y_forward(
                lambda d: cb.at[k, d, j, :, part(q)], lambda d: rl2.at[k, d, j, :, part(q)],
                f2_ss, y2_rs.at[k, q],
            )

    along = [wrap(z + o, NZ) for o in range(NZ)]

    def r_hop(k, q, h):
        s = 1 - 2 * q
        cols = part(q)
        if h >= 2:
            got(rsb.at[k, :, h - 2, :, cols], r_rs.at[k, q, h - 2])
        for way, t, step in ((0, (5 - h) * s, s), (1, (h - 4) * s, -s)):
            if h == 4 and way == 1:
                continue
            t = along[t % NZ]
            if h >= 2:
                held = xb[k, t, :, cols].astype(F32) + rsb[k, way, h - 2, :, cols].astype(F32)
                xb[k, t, :, cols] = held.astype(BF16)
            to = (x, y, along[step % NZ], c)
            rcopy(
                xb.at[k, t, :, cols], rsb.at[k, way, h - 1, :, cols], r_ss, r_rs.at[k, q, h - 1], to
            ).start()

    def combine(k, q):
        got(cb.at[k, pl.ds(0, NS - 1), :, :, part(q)], y2_rs.at[k, q])
        for pair in range(NZ // 2):
            served = cb[k, :, :, 16 * pair : 16 * pair + SPAN, part(q)].reshape(NS * PER * SPAN, thin)
            rows = ws[pair].reshape(4 * tok, NS * PER * SPAN)
            summed = jnp.dot(rows, served, preferred_element_type=F32)
            summed = summed[: 2 * tok] + summed[2 * tok :]
            xb[k, 2 * pair : 2 * pair + 2, :, part(q)] = summed.astype(BF16).reshape(2, tok, thin)
        r_hop(k, q, 1)

    def out_copy(k, q):
        at = pl.ds(pl.multiple_of(k * width + q * thin, thin), thin)
        return pltpu.make_async_copy(outb.at[k, :, part(q)], out_ref.at[:, at], out_s)

    def finish(k, q):
        cols = part(q)
        got(rsb.at[k, 0, 3, :, cols], r_rs.at[k, q, 3])
        value = xb[k, z, :, cols].astype(F32) + rsb[k, 0, 3, :, cols].astype(F32)
        value += rsb[k, 1, 2, :, cols].astype(F32)
        outb[k, :, cols] = value.astype(BF16)
        out_copy(k, q).start()

    total_copy = pltpu.make_async_copy(ctotal, cnt_ref, tot_s)

    @pl.loop(0, NC + 5)
    def _(i):
        guarded(i - 1, lambda k: pass_back(k, 0))
        guarded(i - 3, lambda k: r_hop(k, 0, 2))
        guarded(i - 4, lambda k: r_hop(k, 1, 3))
        guarded(i, lambda k: d_relay(k, 1))
        guarded(i + 1, lambda k: d_own(k, 1), 1)
        guarded(i, lambda k: down(k, 0))
        guarded(i - 2, lambda k: combine(k, 0))
        guarded(i - 5, lambda k: finish(k, 0))
        guarded(i - 3, lambda k: r_hop(k, 1, 2))

        guarded(i - 1, lambda k: pass_back(k, 1))
        guarded(i - 2, lambda k: combine(k, 1))
        guarded(i - 4, lambda k: r_hop(k, 0, 4))
        guarded(i - 5, lambda k: finish(k, 1))
        guarded(i + 1, lambda k: d_relay(k, 0), 1)
        guarded(i + 2, lambda k: d_own(k, 0), 2)
        guarded(i, lambda k: down(k, 1))
        guarded(i - 3, lambda k: r_hop(k, 0, 3))
        guarded(i - 4, lambda k: r_hop(k, 1, 4))

        @pl.when(i == 2)
        def _():
            c_step(4)

        @pl.when(i == NC - 1)
        def _():
            c_step(5)

        @pl.when(i == NC + 1)
        def _():
            total_copy.start()

    sent(wgu.at[:, :, pl.ds(0, NX - 1)], g_ss)
    sent(wdn.at[:, :, pl.ds(0, NX - 1)], d_ss)
    sent(sb.at[:, pl.ds(0, NS - 1)], y2_ss)
    sent(rl2, f2_ss)
    sent(xb.at[:, pl.ds(0, NZ - 1)], r_ss)
    got(outb, out_s)
    total_copy.wait()


def close(mean_load, experts, mixed_ref, total_ref, bias_ref, out_ref, new_bias_ref, count_ref):
    out_ref[...] = mixed_ref[...]
    totals = total_ref[0:1]
    over = mean_load - experts * totals
    sign = jnp.where(over > 0.0, 1.0, jnp.where(over < 0.0, -1.0, 0.0))
    new_bias_ref[...] = bias_ref[...] + bias_rate * sign
    count_ref[...] = totals.astype(jnp.int32)


def body(tokens, routes, route_weight, bias, w_gate, w_up, w_down):
    tok, feat = tokens.shape
    per, ff, _ = w_gate.shape
    experts = bias.shape[0]
    width = feat // NC
    rows = NS * PER * SLOTS
    vmem, anywhere = pl.BlockSpec(memory_space=pltpu.VMEM), pl.BlockSpec(memory_space=pl.ANY)
    dma = pltpu.SemaphoreType.DMA
    mixed, totals = pl.pallas_call(
        kernel,
        out_shape=(
            jax.ShapeDtypeStruct((tok, feat), BF16),
            jax.ShapeDtypeStruct((8, experts), F32),
        ),
        in_specs=[anywhere, anywhere, anywhere, anywhere, anywhere, anywhere],
        out_specs=(anywhere, anywhere),
        scratch_shapes=[
            pltpu.VMEM((NC, NZ, tok, width), BF16),
            pltpu.VMEM((rows, NZ * tok), BF16),
            pltpu.VMEM((NZ // 2, 2, 2, tok, NS * PER * SPAN), BF16),
            pltpu.VMEM((NC, NS, PER, SLOTS, width), BF16),
            pltpu.VMEM((NC, NS, PER, SLOTS, width), BF16),
            pltpu.VMEM((NC, NS, PER, SLOTS, width), BF16),
            pltpu.VMEM((2, per, NX, ff, feat), BF16),
            pltpu.VMEM((NC, per, NX, ff, width), BF16),
            pltpu.VMEM((per, NX, NS * SLOTS, ff), BF16),
            pltpu.VMEM((NC, 2, PER, SLOTS, width), BF16),
            pltpu.VMEM((NC, 2, PER, SLOTS, width), BF16),
            pltpu.VMEM((NC, 2, 4, tok, width), BF16),
            pltpu.VMEM((NZ, 8, tok), jnp.int32),
            pltpu.VMEM((NZ, 8, tok), F32),
            pltpu.VMEM((NZ, NS * PER, tok), F32),
            pltpu.VMEM((NZ, NS * PER, tok), F32),
            pltpu.VMEM((5, 8, tok), F32),
            pltpu.VMEM((5, 8, tok), F32),
            pltpu.VMEM((8, tok), F32),
            pltpu.VMEM((NC, tok, width), BF16),
            dma((4,)),
            dma((2,)),
            dma,
            dma,
            dma,
            dma((2,)),
            dma((2, 4)),
            dma((5,)),
            dma((5,)),
            dma,
            dma((NC, 4)),
            dma,
            dma((NC,)),
            dma((NC,)),
            dma,
            dma,
            dma((NC, PARTS)),
            dma((NC, PER)),
            dma,
            dma,
            dma((NC, PARTS, 4)),
            dma,
            dma((2, PER, 2)),
            dma,
            dma((NC, PER, 2)),
        ],
        compiler_params=pltpu.CompilerParams(
            collective_id=0, has_side_effects=True, vmem_limit_bytes=67_043_328
        ),
        name="moe_layer",
    )(routes.T, route_weight.T, tokens, w_gate, w_up, w_down)
    everyone = NX * NY * NZ * NCORE
    mixed, new_bias, counts = pl.pallas_call(
        functools.partial(close, float(tok * routes.shape[1] * everyone), float(experts)),
        out_shape=(
            jax.ShapeDtypeStruct((tok, feat), BF16),
            jax.ShapeDtypeStruct((1, experts), F32),
            jax.ShapeDtypeStruct((1, experts), jnp.int32),
        ),
        in_specs=[vmem] * 3,
        out_specs=(vmem,) * 3,
        name="moe_close",
    )(mixed, totals, bias.reshape(1, experts))
    return mixed, new_bias.reshape(experts), counts.reshape(experts)


def solution(mesh):
    torus = Mesh(mesh.devices.reshape(NX, NY, NZ, NCORE), DP_EXPERT)
    placed = (
        P(DP_EXPERT, None),
        P(DP_EXPERT, None),
        P(DP_EXPERT, None),
        P(),
        P(EXPERT, "dp", None),
        P(EXPERT, "dp", None),
        P(EXPERT, "dp", None),
    )
    return jax.shard_map(
        body, mesh=torus, in_specs=placed, out_specs=(P(DP_EXPERT, None), P(), P()), check_vma=False
    )
```
